128 devices in a mesh: row: 16 (over y_lo, z, core), col: 8 (over x, y_hi).
Axes of the slice: x: 4, y: 4 (y_hi: 2, y_lo: 2; y = y_hi * 2 + y_lo), z: 4, core: 2. Of those that a mesh axis runs over, the one named last changes fastest.
Arguments:
- ladder_ints: float32 [19712, 19712], P('row', 'col'), may hold values from -0.0390625 to 0.0390625
- amplitudes: float32 [19712, 2048], P('row', 'col'), may hold values from -6 to 6
- phase_map: int32 [16], replicated, may hold values from 0 to 15, each once
Outputs:
- ladder_term: float32 [19712, 2048], P('row', 'col')
The draws below stay inside these ranges and needn't reach their ends.
Inputs may be any that keep to these rules, and one draw needn't show every extreme that they name: `phase_map`: each phase appears once.
All inputs are finite; a program needn't handle non-finite values.
Results may differ from the reference program's by a relative error of at most 0.000078.
Values sent between devices are 32-bit elements; how exact they have to be, the bound alone decides.
A program may use at most 320 MiB of HBM per device.

```python
import jax
import jax.numpy as jnp
from jax import lax

PAIRS = 19712
OCC_PAIRS = 2048
PHASES = 16
N_ROW = 16


def shard_levels(own_key, extent, shards, low, top_value):
    factor_of, own = 1.0, jax.random.fold_in(own_key, 6)
    for axis_at, shards_of in shards:
        draws = jnp.exp(jax.random.uniform(jax.random.fold_in(own, axis_at), (shards_of,), jnp.float32, low / len(shards), top_value / len(shards)))
        factor_of = factor_of * jnp.repeat(draws, extent[axis_at] // shards_of).reshape([-1 if axis == axis_at else 1 for axis in range(len(extent))])
    return factor_of


def gaussian(key, dims, scale, limit, split=(), kind=jnp.bfloat16):
    array = jax.random.normal(key, dims, jnp.float32) * scale
    if len(split) > 0:
        array = shard_levels(key, dims, split, -0.22, 0.18) * array
    return jnp.clip(array, min=-limit, max=limit).astype(kind)


def setup_inputs(seed: int = 0) -> dict:
    streams_of = jax.random.split(jax.random.key(seed), 4)
    ladder_ints = gaussian(streams_of[0], (PAIRS, PAIRS), PAIRS ** -0.5, 0.0390625, ((0, 16), (1, 8)), jnp.float32)
    amplitudes = gaussian(streams_of[1], (PAIRS, OCC_PAIRS), 1.0, 6.0, ((0, 16), (1, 8)), jnp.float32)
    phase_map = jax.random.permutation(streams_of[2], N_ROW).astype(jnp.int32)
    return {"ladder_ints": ladder_ints, "amplitudes": amplitudes, "phase_map": phase_map}


def reference(ladder_ints, amplitudes, phase_map):
    block = PAIRS // PHASES
    inverse = jnp.zeros((PHASES,), jnp.int32).at[phase_map.astype(jnp.int32)].set(jnp.arange(PHASES, dtype=jnp.int32))
    shaped = amplitudes.reshape(PHASES, block, OCC_PAIRS)
    by_phase = jnp.take(shaped, inverse, axis=0)
    ordered = jnp.transpose(by_phase, (1, 0, 2)).reshape(PAIRS, OCC_PAIRS)
    return jnp.dot(ladder_ints, ordered, precision=lax.Precision.HIGHEST, preferred_element_type=jnp.float32)
```

```python
import jax
import jax.numpy as jnp
from jax import lax
from jax.experimental import pallas as pl
from jax.experimental.pallas import tpu as pltpu
from jax.sharding import PartitionSpec as P

UNITS = ((2, 1), (2, 0), (1, 1), (3, 1), (0, 1), (1, 0), (3, 0), (0, 0))
N_UNITS = 8
KPAD = 160
KTOT = 16 * KPAD
NB = 256
MESH = pl.DeviceIdType.MESH


def kernel(rows, depth, v_hbm, a_ref, perm_ref, out_hbm,
           T, Vh, Vl, Th, Tl, Pt, RA, RD, RY, Vs,
           arecv, asend, yrecv, ysend, zrecv, zsend, frecv, fsend, drecv, dsend,
           hrecv, hsend, xrecv, xsend, rysem, vsem, osem):
    r = lax.axis_index("row")
    c = lax.axis_index("col")
    x = c // 2
    yh = c % 2
    yl = r // 8
    z = (r // 2) % 4
    core = r % 2
    half = rows // 2

    def col_of(dx, other):
        return ((x + dx) % 4) * 2 + (yh + other) % 2

    def row_of(other):
        return ((yl + other) % 2) * 8 + z * 2 + core

    row_y = ((yl + 1) % 2) * 8 + z * 2 + core
    row_zp = yl * 8 + ((z + 1) % 4) * 2 + core
    row_zm = yl * 8 + ((z + 3) % 4) * 2 + core
    row_c = yl * 8 + z * 2 + (core + 1) % 2
    zm = (z + 3) % 4
    zp = (z + 1) % 4
    z2 = (z + 2) % 4

    def remote(src, dst, ssem, rsem, row, col):
        return pltpu.make_async_remote_copy(
            src_ref=src, dst_ref=dst, send_sem=ssem, recv_sem=rsem,
            device_id={"row": row, "col": col}, device_id_type=MESH)

    barrier = pltpu.get_barrier_semaphore()
    peers = [(row_of(o), col_of(dx, o)) for dx, o in UNITS if (dx, o) != (0, 0)]
    peers += [(row_y, c), (row_zp, c), (row_zm, c), (row_c, c), (r, col_of(0, 1))]
    for pr, pc in peers:
        pl.semaphore_signal(barrier, inc=1, device_id={"row": pr, "col": pc}, device_id_type=MESH)

    RT = Vs.shape[1]
    n_rt = rows // RT

    def v_copy(i, slot):
        return pltpu.make_async_copy(v_hbm.at[pl.ds(i * RT, RT), :], Vs.at[slot], vsem.at[slot])

    v_copy(0, 0).start()
    pl.semaphore_wait(barrier, len(peers))

    def slot_src(u):
        return core * 8 + z * 2 + (yl + UNITS[u][1]) % 2

    def a2a(u):
        dx, o = UNITS[u]
        dcol = col_of(4 - dx, o)
        return remote(a_ref.at[dcol], T.at[u, core * 8 + z * 2 + yl], asend.at[u], arecv.at[u], row_of(o), dcol)

    def a2a_in(u):
        return remote(a_ref.at[0], T.at[u, slot_src(u)], asend.at[u], arecv.at[u], r, c)

    def ycopy(u):
        s = slot_src(u)
        return remote(T.at[u, s], T.at[u, s], ysend.at[u], yrecv.at[u], row_y, c)

    def pair(u, zz):
        return T.at[u, pl.ds(core * 8 + zz * 2, 2)]

    def zcopy(u, way):
        return remote(pair(u, z), pair(u, z), zsend.at[u, way], zrecv.at[u, way], (row_zp, row_zm)[way], c)

    def fcopy(u, way):
        s = core * 8 + (zm, zp)[way] * 2 + way
        return remote(T.at[u, s], T.at[u, s], fsend.at[u, way], frecv.at[u, way], (row_zp, row_zm)[way], c)

    def dcopy(u, i):
        p = pair(u, (z, zm, zp, z2)[i])
        return remote(p, p, dsend.at[u, i], drecv.at[u, i], row_c, c)

    def S1(u):
        if u < N_UNITS - 1:
            a2a_in(u).wait_recv()
        ycopy(u).start()

    def S2(u):
        ycopy(u).wait_recv()
        zcopy(u, 0).start()
        zcopy(u, 1).start()
        dcopy(u, 0).start()

    def S3(u):
        for way in (0, 1):
            zcopy(u, way).wait_recv()
            fcopy(u, way).start()
        dcopy(u, 1).start()
        dcopy(u, 2).start()

    def S4(u):
        fcopy(u, 0).wait_recv()
        fcopy(u, 1).wait_recv()
        dcopy(u, 3).start()

    def S5(u):
        for i in range(4):
            dcopy(u, i).wait_recv()

    def vprep(lo, hi):
        @pl.loop(lo, hi)
        def _(i):
            slot = i % 2

            @pl.when(i + 1 < n_rt)
            def _():
                v_copy(i + 1, (i + 1) % 2).start()

            v_copy(i, slot).wait()
            rs = pl.ds(pl.multiple_of(i * RT, RT), RT)
            for j in range(KTOT // 256):
                w = min(256, depth - j * 256)
                v = Vs[slot, :, j * 256:j * 256 + w]
                h = v.astype(jnp.bfloat16)
                l = (v - h.astype(jnp.float32)).astype(jnp.bfloat16)
                p = perm_ref[0:w, :]
                Vh[rs, j * 256:(j + 1) * 256] = jnp.dot(h, p, preferred_element_type=jnp.float32).astype(jnp.bfloat16)
                Vl[rs, j * 256:(j + 1) * 256] = jnp.dot(l, p, preferred_element_type=jnp.float32).astype(jnp.bfloat16)

    def prep(u):
        @pl.loop(0, KPAD // 8)
        def _(kb):
            t = T[u, :, pl.ds(pl.multiple_of(kb * 8, 8), 8), :].reshape(128, NB)
            h = t.astype(jnp.bfloat16)
            ks = pl.ds(pl.multiple_of(kb * 128, 128), 128)
            Th[ks, :] = h
            Tl[ks, :] = (t - h.astype(jnp.float32)).astype(jnp.bfloat16)

    MT = 176

    def mm(u, lo, hi):
        @pl.loop(lo, hi)
        def _(i):
            rs = pl.ds(pl.multiple_of(i * MT, MT), MT)
            vh = Vh[rs, :]
            acc = jnp.dot(vh, Tl[...], preferred_element_type=jnp.float32)
            acc += jnp.dot(Vl[rs, :], Th[...], preferred_element_type=jnp.float32)
            acc += jnp.dot(vh, Th[...], preferred_element_type=jnp.float32)
            Pt[u, rs, :] = acc

    def add(dst, srcs, n):
        @pl.loop(0, n // 56)
        def _(i):
            rs = pl.ds(pl.multiple_of(i * 56, 8), 56)
            t = dst[rs, :]
            for s in srcs:
                t = t + s[rs, :]
            dst[rs, :] = t

    def half_copy(h, way):
        u = (0, 1)[1 - h]
        return remote(Pt.at[u, pl.ds(way * half, half)], RA.at[h * 2 + way],
                      hsend.at[h * 2 + way], hrecv.at[h * 2 + way], r, col_of((1, 3)[way], 0))

    def full_copy(h, way):
        u = UNITS.index(((1, 3)[way], h))
        return remote(Pt.at[u], RD.at[h * 2 + way], xsend.at[h * 2 + way], xrecv.at[h * 2 + way],
                      r, col_of((1, 3)[way], 0))

    def last_copy():
        return remote(Pt.at[UNITS.index((0, 1))], RY, rysem.at[0], rysem.at[1], r, col_of(0, 1))

    def reduce_step(u):
        dx, h = UNITS[u]
        if dx == 2:
            half_copy(h, 0).start()
            half_copy(h, 1).start()
        elif dx in (1, 3):
            way = 0 if dx == 1 else 1
            half_copy(h, way).wait_recv()
            add(Pt.at[u, pl.ds(way * half, half)], [RA.at[h * 2 + way]], half)
            full_copy(h, way).start()

    def finish(h):
        u = UNITS.index((0, h))
        full_copy(h, 0).wait_recv()
        full_copy(h, 1).wait_recv()
        srcs = [RD.at[h * 2], RD.at[h * 2 + 1]]
        if h == 0:
            last_copy().wait_recv()
            srcs.append(RY)
        add(Pt.at[u], srcs, rows)
        if h == 1:
            last_copy().start()

    for u in range(N_UNITS - 1):
        a2a(u).start()
    T[N_UNITS - 1, core * 8 + z * 2 + yl] = a_ref[c]

    vprep(0, 2)
    S1(0)
    S1(1)
    vprep(2, 4)
    S2(0)
    S1(2)
    vprep(4, 5)
    S2(1)
    S1(3)
    vprep(5, 6)
    S3(0)
    vprep(6, 7)
    S2(2)
    S1(4)
    S3(1)
    S4(0)
    for u in range(N_UNITS):
        S5(u)
        prep(u)
        if u + 5 < N_UNITS:
            S1(u + 5)
        if u + 3 < N_UNITS:
            S2(u + 3)
        mm(u, 0, 4)
        if u + 2 < N_UNITS:
            S3(u + 2)
        mm(u, 4, 7)
        if u + 1 < N_UNITS:
            S4(u + 1)
        reduce_step(u)
        if UNITS[u] == (1, 0):
            finish(1)
    finish(0)
    o = pltpu.make_async_copy(Pt.at[N_UNITS - 1], out_hbm, osem)
    o.start()
    o.wait()
    for u in range(N_UNITS):
        if u < N_UNITS - 1:
            a2a(u).wait_send()
        ycopy(u).wait_send()
        for way in (0, 1):
            zcopy(u, way).wait_send()
            fcopy(u, way).wait_send()
        for i in range(4):
            dcopy(u, i).wait_send()
    for h in (0, 1):
        for way in (0, 1):
            half_copy(h, way).wait_send()
            full_copy(h, way).wait_send()
    last_copy().wait_send()


def per_device(ladder_ints, amplitudes, phase_map):
    rows, depth = ladder_ints.shape
    kb = depth // 16
    a = jnp.pad(amplitudes.reshape(8, kb, NB), ((0, 0), (0, KPAD - kb), (0, 0)))
    slot_phase = phase_map.reshape(2, 4, 2).transpose(2, 1, 0).reshape(16)
    src = jnp.arange(256)
    dst = jnp.arange(256)
    want = (dst // 128) * 128 + (dst % 8) * 16 + jnp.repeat(jnp.tile(slot_phase, 2), 8)
    perm = (src[:, None] == want[None, :]).astype(jnp.bfloat16)
    f32, bf16 = jnp.float32, jnp.bfloat16
    dma = pltpu.SemaphoreType.DMA
    import functools
    return pl.pallas_call(
        functools.partial(kernel, rows, depth),
        out_shape=jax.ShapeDtypeStruct((rows, NB), f32),
        in_specs=[pl.BlockSpec(memory_space=pl.ANY), pl.BlockSpec(memory_space=pltpu.VMEM),
                  pl.BlockSpec(memory_space=pltpu.VMEM)],
        out_specs=pl.BlockSpec(memory_space=pl.ANY),
        scratch_shapes=[
            pltpu.VMEM((N_UNITS, 16, KPAD, NB), f32),
            pltpu.VMEM((rows, KTOT), bf16),
            pltpu.VMEM((rows, KTOT), bf16),
            pltpu.VMEM((KTOT, NB), bf16),
            pltpu.VMEM((KTOT, NB), bf16),
            pltpu.VMEM((N_UNITS, rows, NB), f32),
            pltpu.VMEM((4, rows // 2, NB), f32),
            pltpu.VMEM((4, rows, NB), f32),
            pltpu.VMEM((rows, NB), f32),
            pltpu.VMEM((2, 176, depth), f32),
            dma((8,)), dma((8,)), dma((8,)), dma((8,)), dma((8, 2)), dma((8, 2)), dma((8, 2)), dma((8, 2)),
            dma((8, 4)), dma((8, 4)), dma((4,)), dma((4,)), dma((4,)), dma((4,)), dma((2,)), dma((2,)), dma,
        ],
        compiler_params=pltpu.CompilerParams(
            collective_id=0, has_side_effects=True, vmem_limit_bytes=67043328),
        name="ladder",
    )(ladder_ints, a, perm)


def solution(mesh):
    in_specs = (P("row", "col"), P("row", "col"), P())
    out_specs = P("row", "col")
    return jax.shard_map(
        per_device, mesh=mesh, in_specs=in_specs, out_specs=out_specs, check_vma=False
    )
```

```python
import functools

import jax
import jax.numpy as jnp
from jax import lax
from jax.experimental import pallas as pl
from jax.experimental.pallas import tpu as pltpu
from jax.sharding import PartitionSpec as P

UNITS = ((2, 1), (2, 0), (1, 1), (3, 1), (1, 0), (3, 0), (0, 1), (0, 0))
N_UNITS = 8
KPAD = 160
KTOT = 16 * KPAD
NB = 256
RT = 176
CUT = (3, 4)
MESH = pl.DeviceIdType.MESH


def kernel(rows, depth, v_hbm, amp, phase, out_s, out_y,
           apad, perm, T, Vh, Vl, Th, Tl, Pt, RA, RD, RY, Vs,
           arecv, asend, yrecv, ysend, zrecv, zsend, frecv, fsend, drecv, dsend,
           hrecv, hsend, xrecv, xsend, lrecv, lsend, vsem, osem):
    r = lax.axis_index("row")
    c = lax.axis_index("col")
    x = c // 2
    yh = c % 2
    yl = r // 8
    z = (r // 2) % 4
    core = r % 2
    kb = depth // 16
    n_rt = rows // RT

    def col_of(dx, other):
        return ((x + dx) % 4) * 2 + (yh + other) % 2

    def row_of(other):
        return ((yl + other) % 2) * 8 + z * 2 + core

    row_y = row_of(1)
    zs = (z, (z + 3) % 4, (z + 1) % 4, (z + 2) % 4)
    row_zp = yl * 8 + zs[2] * 2 + core
    row_zm = yl * 8 + zs[1] * 2 + core
    row_z = (row_zp, row_zm)
    row_c = yl * 8 + z * 2 + (core + 1) % 2

    def remote(src, dst, ssem, rsem, row, col):
        return pltpu.make_async_remote_copy(
            src_ref=src, dst_ref=dst, send_sem=ssem, recv_sem=rsem,
            device_id={"row": row, "col": col}, device_id_type=MESH)

    barrier = pltpu.get_barrier_semaphore()
    peers = [(row_of(o), col_of(dx, o)) for dx, o in UNITS if (dx, o) != (0, 0)]
    peers += [(row_y, c), (row_zp, c), (row_zm, c), (row_c, c), (r, col_of(0, 1))]
    for pr, pc in peers:
        pl.semaphore_signal(barrier, inc=1, device_id={"row": pr, "col": pc}, device_id_type=MESH)

    def v_copy(i, slot):
        return pltpu.make_async_copy(v_hbm.at[pl.ds(i * RT, RT), :], Vs.at[slot], vsem.at[slot])

    def own(u):
        return (yl + UNITS[u][1]) % 2

    def slot(zz, ys):
        return core * 8 + zz * 2 + ys

    def a2a(u):
        dx, o = UNITS[u]
        dcol = col_of(4 - dx, o)
        return remote(apad.at[dcol], T.at[u, slot(z, yl)], asend.at[u], arecv.at[u], row_of(o), dcol)

    def a2a_in(u):
        return remote(apad.at[0], T.at[u, slot(z, own(u))], asend.at[u], arecv.at[u], r, c)

    def ycopy(u, i):
        ref = T.at[u, slot(zs[3 * i], own(u))]
        return remote(ref, ref, ysend.at[u, i], yrecv.at[u, i], row_y, c)

    def ycopy_in(u, i):
        ref = T.at[u, slot(zs[3 * i], 1 - own(u))]
        return remote(ref, ref, ysend.at[u, i], yrecv.at[u, i], row_y, c)

    def zcopy(u, way, k):
        ref = T.at[u, slot(z, (own(u) + k) % 2)]
        return remote(ref, ref, zsend.at[u, way * 2 + k], zrecv.at[u, way * 2 + k], row_z[way], c)

    def zcopy_in(u, way, k):
        ref = T.at[u, slot(zs[1 + way], (own(u) + k) % 2)]
        return remote(ref, ref, zsend.at[u, way * 2 + k], zrecv.at[u, way * 2 + k], row_z[way], c)

    hk = KPAD // 2

    def fcopy(u, way):
        ref = T.at[u, slot(zs[1 + way], own(u)), pl.ds(way * hk, hk)]
        return remote(ref, ref, fsend.at[u, way], frecv.at[u, way], row_z[way], c)

    def fcopy_in(u, way):
        ref = T.at[u, slot(zs[3], own(u)), pl.ds(way * hk, hk)]
        return remote(ref, ref, fsend.at[u, way], frecv.at[u, way], row_z[way], c)

    def dcopy(u, i):
        ref = T.at[u, pl.ds(core * 8 + zs[i] * 2, 2)]
        return remote(ref, ref, dsend.at[u, i], drecv.at[u, i], row_c, c)

    def dcopy_in(u, i):
        ref = T.at[u, pl.ds((1 - core) * 8 + zs[i] * 2, 2)]
        return remote(ref, ref, dsend.at[u, i], drecv.at[u, i], row_c, c)

    def E1(u):
        if UNITS[u] != (0, 0):
            a2a_in(u).wait_recv()
        zcopy(u, 0, 0).start()
        zcopy(u, 1, 0).start()
        ycopy(u, 0).start()

    def E2(u):
        ycopy_in(u, 0).wait_recv()
        zcopy(u, 0, 1).start()
        zcopy(u, 1, 1).start()
        dcopy(u, 0).start()

    def E3(u):
        for way in (0, 1):
            zcopy_in(u, way, 0).wait_recv()
            fcopy(u, way).start()

    def E4(u):
        fcopy_in(u, 0).wait_recv()
        fcopy_in(u, 1).wait_recv()
        ycopy(u, 1).start()

    def E5(u):
        for way in (0, 1):
            zcopy_in(u, way, 1).wait_recv()
            dcopy(u, 1 + way).start()

    def E6(u):
        ycopy_in(u, 1).wait_recv()
        dcopy(u, 3).start()

    def E7(u):
        for i in range(4):
            dcopy_in(u, i).wait_recv()

    def vprep(lo, hi):
        @pl.loop(lo, hi)
        def _(i):
            s = i % 2

            @pl.when(i + 1 < n_rt)
            def _():
                v_copy(i + 1, (i + 1) % 2).start()

            v_copy(i, s).wait()
            rs = pl.ds(pl.multiple_of(i * RT, RT), RT)
            for j in range(KTOT // 256):
                w = min(256, depth - j * 256)
                v = Vs[s, :, j * 256:j * 256 + w]
                h = v.astype(jnp.bfloat16)
                l = (v - h.astype(jnp.float32)).astype(jnp.bfloat16)
                p = perm[0:w, :]
                Vh[rs, j * 256:(j + 1) * 256] = jnp.dot(h, p, preferred_element_type=jnp.float32).astype(jnp.bfloat16)
                Vl[rs, j * 256:(j + 1) * 256] = jnp.dot(l, p, preferred_element_type=jnp.float32).astype(jnp.bfloat16)

    def aprep():
        for j in range(8):
            apad[j, 0:kb, :] = amp[j * kb:(j + 1) * kb, :]
            apad[j, kb:KPAD, :] = jnp.zeros((KPAD - kb, NB), jnp.float32)

    def permprep():
        lane = lax.broadcasted_iota(jnp.int32, (1, 256), 1)
        want = (lane // 128) * 128 + (lane % 8) * 16
        which = (lane % 128) // 8
        for s in range(16):
            g = (s % 2) * 8 + ((s // 2) % 4) * 2 + s // 8
            want = want + jnp.where(which == s, phase[g], 0)
        rowi = lax.broadcasted_iota(jnp.int32, (256, 256), 0)
        perm[...] = jnp.where(rowi == want, 1.0, 0.0).astype(jnp.bfloat16)

    def prep(u):
        @pl.loop(0, KPAD // 8)
        def _(k):
            t = T[u, :, pl.ds(pl.multiple_of(k * 8, 8), 8), :].reshape(128, NB)
            h = t.astype(jnp.bfloat16)
            ks = pl.ds(pl.multiple_of(k * 128, 128), 128)
            Th[ks, :] = h
            Tl[ks, :] = (t - h.astype(jnp.float32)).astype(jnp.bfloat16)

    def mm(u, lo, hi):
        @pl.loop(lo, hi)
        def _(i):
            rs = pl.ds(pl.multiple_of(i * RT, RT), RT)
            vh = Vh[rs, :]
            acc = jnp.dot(vh, Tl[...], preferred_element_type=jnp.float32)
            acc += jnp.dot(Vl[rs, :], Th[...], preferred_element_type=jnp.float32)
            acc += jnp.dot(vh, Th[...], preferred_element_type=jnp.float32)
            Pt[u, rs, :] = acc

    def add(dst, srcs, lo, n, off=0):
        @pl.loop(0, n // 88)
        def _(i):
            rs = pl.ds(pl.multiple_of(lo + i * 88, 8), 88)
            t = dst[rs, :]
            for s in srcs:
                t = t + s[pl.ds(pl.multiple_of(lo - off + i * 88, 8), 88), :]
            dst[rs, :] = t

    def part(h, k):
        cut = CUT[h] * RT
        return (0, cut) if k == 0 else (cut, rows - cut)

    def half_copy(h, way):
        lo, n = part(h, way)
        return remote(Pt.at[UNITS.index((2, h)), pl.ds(lo, n)], RA.at[h * 2 + way, pl.ds(0, n)],
                      hsend.at[h * 2 + way], hrecv.at[h * 2 + way], r, col_of((1, 3)[way], 0))

    def full_copy(h, way, k):
        lo, n = part(h, k)
        u = UNITS.index(((1, 3)[way], h))
        i = h * 2 + way
        return remote(Pt.at[u, pl.ds(lo, n)], RD.at[i, pl.ds(lo, n)], xsend.at[i, k], xrecv.at[i, k],
                      r, col_of((1, 3)[way], 0))

    def last_copy(k):
        lo, n = part(1, k)
        return remote(Pt.at[UNITS.index((0, 1)), pl.ds(lo, n)], RY.at[pl.ds(lo, n)], lsend.at[k], lrecv.at[k],
                      r, col_of(0, 1))

    def reduce_step(u, k):
        dx, h = UNITS[u]
        if dx == 2:
            half_copy(h, k).start()
        elif dx in (1, 3):
            way = 0 if dx == 1 else 1
            if way == k:
                half_copy(h, way).wait_recv()
                lo, n = part(h, k)
                add(Pt.at[u], [RA.at[h * 2 + way]], lo, n, lo)
            full_copy(h, way, k).start()

    def finish(h, k):
        u = UNITS.index((0, h))
        lo, n = part(h, k)
        full_copy(h, 0, k).wait_recv()
        full_copy(h, 1, k).wait_recv()
        add(Pt.at[u], [RD.at[h * 2], RD.at[h * 2 + 1]], lo, n)
        if h == 1:
            last_copy(k).start()
        else:
            out_copy(k).start()

    def out_copy(k):
        lo, n = part(0, k)
        return pltpu.make_async_copy(Pt.at[UNITS.index((0, 0)), pl.ds(lo, n)], out_s.at[pl.ds(lo, n)], osem.at[k])

    y_copy = pltpu.make_async_copy(RY, out_y, osem.at[2])

    def unit(u):
        E7(u)
        prep(u)
        cut = CUT[UNITS[u][1]]
        mm(u, 0, 2)
        if u + 1 < N_UNITS:
            E4(u + 1)
            E5(u + 1)
        mm(u, 2, cut)
        reduce_step(u, 0)
        if u + 2 < N_UNITS:
            E2(u + 2)
            E3(u + 2)
        if u + 3 < N_UNITS:
            E1(u + 3)
        mm(u, cut, n_rt)
        reduce_step(u, 1)
        if u + 1 < N_UNITS:
            E6(u + 1)

    v_copy(0, 0).start()
    aprep()
    permprep()
    vprep(0, 1)
    pl.semaphore_wait(barrier, len(peers))
    a2a(0).start()
    a2a(1).start()
    T[N_UNITS - 1, slot(z, yl)] = apad[c]
    vprep(1, 3)
    for u in range(2, N_UNITS - 1):
        a2a(u).start()
    E1(0)
    vprep(3, 5)
    E2(0)
    E3(0)
    E1(1)
    vprep(5, 7)
    E5(0)
    E4(0)
    E2(1)
    E3(1)
    E1(2)
    E6(0)
    for u in range(N_UNITS):
        unit(u)
        if UNITS[u] == (0, 1):
            finish(1, 0)
            finish(1, 1)
    last_copy(0).wait_recv()
    last_copy(1).wait_recv()
    y_copy.start()
    finish(0, 0)
    finish(0, 1)
    for u in range(N_UNITS):
        if UNITS[u] != (0, 0):
            a2a(u).wait_send()
        for i in (0, 1):
            ycopy(u, i).wait_send()
            fcopy(u, i).wait_send()
            for k in (0, 1):
                zcopy(u, i, k).wait_send()
        for i in range(4):
            dcopy(u, i).wait_send()
    for k in (0, 1):
        for h in (0, 1):
            half_copy(h, k).wait_send()
            for way in (0, 1):
                full_copy(h, way, k).wait_send()
        last_copy(k).wait_send()
        out_copy(k).wait()
    y_copy.wait()


def per_device(ladder_ints, amplitudes, phase_map):
    rows, depth = ladder_ints.shape
    f32, bf16 = jnp.float32, jnp.bfloat16
    dma = pltpu.SemaphoreType.DMA
    out = jax.ShapeDtypeStruct((rows, NB), f32)
    s, y = pl.pallas_call(
        functools.partial(kernel, rows, depth),
        out_shape=(out, out),
        in_specs=[pl.BlockSpec(memory_space=pl.ANY), pl.BlockSpec(memory_space=pltpu.VMEM),
                  pl.BlockSpec(memory_space=pltpu.SMEM)],
        out_specs=(pl.BlockSpec(memory_space=pl.ANY), pl.BlockSpec(memory_space=pl.ANY)),
        scratch_shapes=[
            pltpu.VMEM((8, KPAD, NB), f32),
            pltpu.VMEM((256, 256), bf16),
            pltpu.VMEM((N_UNITS, 16, KPAD, NB), f32),
            pltpu.VMEM((rows, KTOT), bf16),
            pltpu.VMEM((rows, KTOT), bf16),
            pltpu.VMEM((KTOT, NB), bf16),
            pltpu.VMEM((KTOT, NB), bf16),
            pltpu.VMEM((N_UNITS, rows, NB), f32),
            pltpu.VMEM((4, max(CUT) * RT, NB), f32),
            pltpu.VMEM((4, rows, NB), f32),
            pltpu.VMEM((rows, NB), f32),
            pltpu.VMEM((2, RT, depth), f32),
            dma((8,)), dma((8,)), dma((8, 2)), dma((8, 2)), dma((8, 4)), dma((8, 4)), dma((8, 2)), dma((8, 2)),
            dma((8, 4)), dma((8, 4)), dma((4,)), dma((4,)), dma((4, 2)), dma((4, 2)), dma((2,)), dma((2,)),
            dma((2,)), dma((3,)),
        ],
        compiler_params=pltpu.CompilerParams(
            collective_id=0, has_side_effects=True, vmem_limit_bytes=67043328),
        name="ladder",
    )(ladder_ints, amplitudes, phase_map)
    return s + y


def solution(mesh):
    in_specs = (P("row", "col"), P("row", "col"), P())
    out_specs = P("row", "col")
    return jax.shard_map(
        per_device, mesh=mesh, in_specs=in_specs, out_specs=out_specs, check_vma=False
    )
```

```python
import functools

import jax
import jax.numpy as jnp
from jax import lax
from jax.experimental import pallas as pl
from jax.experimental.pallas import tpu as pltpu
from jax.sharding import PartitionSpec as P

UNITS = (("A", 1, 0), ("A", 0, 0), ("M", 1, 0), ("M", 1, 1), ("M", 0, 0), ("D", 1, 0), ("M", 0, 1), ("D", 0, 0))
N_UNITS = 8
KPAD = 160
KTOT = 16 * KPAD
NB = 256
HB = NB // 2
RT = 176
CUT = 4
STEPS = ((0, 0, KPAD // 2), (0, KPAD // 2, KPAD // 2)) + tuple((u, 0, KPAD) for u in range(1, N_UNITS))
NO_Y2 = (0, 1, 8)
CHUNKS = (((0, RT), (2 * RT, RT), (4 * RT, RT), (6 * RT, RT // 2)),
          ((RT, RT), (3 * RT, RT), (5 * RT, RT), (6 * RT + RT // 2, RT // 2)))
MESH = pl.DeviceIdType.MESH


def kernel(rows, depth, v_hbm, amp_hbm, phase, out,
           amp, apad, perm, T, Vh, Vl, Th, Tl, Pt, RA, RD, RY, Vs,
           arecv, asend, yrecv, ysend, zrecv, zsend, frecv, fsend, drecv, dsend,
           hrecv, hsend, xrecv, xsend, lrecv, lsend, vsem, asem):
    r = lax.axis_index("row")
    c = lax.axis_index("col")
    x = c // 2
    yh = c % 2
    yl = r // 8
    z = (r // 2) % 4
    core = r % 2
    kb = depth // 16
    n_rt = rows // RT

    def col_of(dx, other):
        return ((x + dx) % 4) * 2 + (yh + other) % 2

    def row_of(other):
        return ((yl + other) % 2) * 8 + z * 2 + core

    row_y = row_of(1)
    zs = (z, (z + 3) % 4, (z + 1) % 4, (z + 2) % 4)
    row_zp = yl * 8 + zs[2] * 2 + core
    row_zm = yl * 8 + zs[1] * 2 + core
    row_z = (row_zp, row_zm)
    row_c = yl * 8 + z * 2 + (core + 1) % 2

    def remote(src, dst, ssem, rsem, row, col):
        return pltpu.make_async_remote_copy(
            src_ref=src, dst_ref=dst, send_sem=ssem, recv_sem=rsem,
            device_id={"row": row, "col": col}, device_id_type=MESH)

    barrier = pltpu.get_barrier_semaphore()
    peers = [(row_of(o), col_of(dx, o)) for dx in range(4) for o in (0, 1) if (dx, o) != (0, 0)]
    peers += [(row_y, c), (row_zp, c), (row_zm, c), (row_c, c), (r, col_of(0, 1))]
    for pr, pc in peers:
        pl.semaphore_signal(barrier, inc=1, device_id={"row": pr, "col": pc}, device_id_type=MESH)

    def v_copy(i, slot):
        return pltpu.make_async_copy(v_hbm.at[pl.ds(i * RT, RT), :], Vs.at[slot], vsem.at[slot])

    def own(u):
        return (yl + UNITS[u][1]) % 2

    def slot(zz, ys):
        return core * 8 + zz * 2 + ys

    def piece(g, zz, ys):
        u, lo, n = STEPS[g]
        return T.at[u, slot(zz, ys), pl.ds(lo, n)]

    def a2a_parts(g):
        kind, _, p = UNITS[STEPS[g][0]]
        if kind == "M":
            return ((1, p * HB, HB, 0), (3, p * HB, HB, HB))
        return ((2 if kind == "A" else 0, 0, NB, 0),)

    def a2a(g, i):
        u, lo, n = STEPS[g]
        dx, c0, w, d0 = a2a_parts(g)[i]
        o = UNITS[u][1]
        dcol = col_of(4 - dx, o)
        return remote(apad.at[dcol, pl.ds(lo, n), pl.ds(c0, w)],
                      T.at[u, slot(z, yl), pl.ds(lo, n), pl.ds(d0, w)],
                      asend.at[g, i], arecv.at[g, i], row_of(o), dcol)

    def a2a_in(g, i):
        u, lo, n = STEPS[g]
        _, c0, w, d0 = a2a_parts(g)[i]
        return remote(apad.at[0, pl.ds(lo, n), pl.ds(c0, w)],
                      T.at[u, slot(z, own(u)), pl.ds(lo, n), pl.ds(d0, w)],
                      asend.at[g, i], arecv.at[g, i], r, c)

    def send_out(*gs):
        for g in gs:
            for i in range(len(a2a_parts(g))):
                a2a(g, i).start()

    def ycopy(g, i):
        ref = piece(g, zs[3 * i], own(STEPS[g][0]))
        return remote(ref, ref, ysend.at[g, i], yrecv.at[g, i], row_y, c)

    def ycopy_in(g, i):
        ref = piece(g, zs[3 * i], 1 - own(STEPS[g][0]))
        return remote(ref, ref, ysend.at[g, i], yrecv.at[g, i], row_y, c)

    def zcopy(g, way, k):
        ref = piece(g, z, (own(STEPS[g][0]) + k) % 2)
        return remote(ref, ref, zsend.at[g, way * 2 + k], zrecv.at[g, way * 2 + k], row_z[way], c)

    def zcopy_in(g, way, k):
        ref = piece(g, zs[1 + way], (own(STEPS[g][0]) + k) % 2)
        return remote(ref, ref, zsend.at[g, way * 2 + k], zrecv.at[g, way * 2 + k], row_z[way], c)

    def fpart(g, way, zz, k):
        u, lo, n = STEPS[g]
        return T.at[u, slot(zz, (own(u) + k) % 2), pl.ds(lo + way * (n // 2), n // 2)]

    def fcopy(g, way, k=0):
        ref = fpart(g, way, zs[1 + way], k)
        return remote(ref, ref, fsend.at[g, k * 2 + way], frecv.at[g, k * 2 + way], row_z[way], c)

    def fcopy_in(g, way, k=0):
        ref = fpart(g, way, zs[3], k)
        return remote(ref, ref, fsend.at[g, k * 2 + way], frecv.at[g, k * 2 + way], row_z[way], c)

    def dpair(g, i, k):
        u, lo, n = STEPS[g]
        return T.at[u, pl.ds(k * 8 + zs[i] * 2, 2), pl.ds(lo, n)]

    def dcopy(g, i):
        ref = dpair(g, i, core)
        return remote(ref, ref, dsend.at[g, i], drecv.at[g, i], row_c, c)

    def dcopy_in(g, i):
        ref = dpair(g, i, 1 - core)
        return remote(ref, ref, dsend.at[g, i], drecv.at[g, i], row_c, c)

    def local(g):
        return UNITS[STEPS[g][0]][:2] == ("D", 0)

    def Y0(g):
        if not local(g):
            for i in range(len(a2a_parts(g))):
                a2a_in(g, i).wait_recv()
        ycopy(g, 0).start()

    def Z0(g):
        zcopy(g, 0, 0).start()
        zcopy(g, 1, 0).start()

    def E1(g):
        Y0(g)
        Z0(g)

    def E2(g):
        ycopy_in(g, 0).wait_recv()
        zcopy(g, 0, 1).start()
        zcopy(g, 1, 1).start()
        dcopy(g, 0).start()

    def E3(g):
        for way in (0, 1):
            zcopy_in(g, way, 0).wait_recv()
            fcopy(g, way).start()

    def E4(g):
        fcopy_in(g, 0).wait_recv()
        fcopy_in(g, 1).wait_recv()
        if g not in NO_Y2:
            ycopy(g, 1).start()

    def E5(g):
        for way in (0, 1):
            zcopy_in(g, way, 1).wait_recv()
            if g in NO_Y2:
                fcopy(g, way, 1).start()
            dcopy(g, 1 + way).start()

    def E6(g):
        if g in NO_Y2:
            fcopy_in(g, 0, 1).wait_recv()
            fcopy_in(g, 1, 1).wait_recv()
        else:
            ycopy_in(g, 1).wait_recv()
        dcopy(g, 3).start()

    def E7(g):
        for i in range(4):
            dcopy_in(g, i).wait_recv()

    def vprep(lo, hi):
        @pl.loop(lo, hi)
        def _(i):
            s = i % 2

            @pl.when(i + 1 < n_rt)
            def _():
                v_copy(i + 1, (i + 1) % 2).start()

            v_copy(i, s).wait()
            rs = pl.ds(pl.multiple_of(i * RT, RT), RT)
            for j in range(KTOT // 256):
                w = min(256, depth - j * 256)
                v = Vs[s, :, j * 256:j * 256 + w]
                h = v.astype(jnp.bfloat16)
                l = (v - h.astype(jnp.float32)).astype(jnp.bfloat16)
                p = perm[0:w, :]
                Vh[rs, j * 256:(j + 1) * 256] = jnp.dot(h, p, preferred_element_type=jnp.float32).astype(jnp.bfloat16)
                Vl[rs, j * 256:(j + 1) * 256] = jnp.dot(l, p, preferred_element_type=jnp.float32).astype(jnp.bfloat16)

    def aprep():
        for j in range(8):
            apad[j, 0:kb, :] = amp[j * kb:(j + 1) * kb, :]
            apad[j, kb:KPAD, :] = jnp.zeros((KPAD - kb, NB), jnp.float32)

    def permprep():
        lane = lax.broadcasted_iota(jnp.int32, (1, 256), 1)
        want = (lane // 128) * 128 + (lane % 8) * 16
        which = (lane % 128) // 8
        for s in range(16):
            g = (s % 2) * 8 + ((s // 2) % 4) * 2 + s // 8
            want = want + jnp.where(which == s, phase[g], 0)
        rowi = lax.broadcasted_iota(jnp.int32, (256, 256), 0)
        perm[...] = jnp.where(rowi == want, 1.0, 0.0).astype(jnp.bfloat16)

    def prep(g):
        u, first, n = STEPS[g]

        @pl.loop(first // 8, (first + n) // 8)
        def _(k):
            t = T[u, :, pl.ds(pl.multiple_of(k * 8, 8), 8), :].reshape(128, NB)
            h = t.astype(jnp.bfloat16)
            ks = pl.ds(pl.multiple_of(k * 128, 128), 128)
            Th[ks, :] = h
            Tl[ks, :] = (t - h.astype(jnp.float32)).astype(jnp.bfloat16)

    def mm(u, lo, hi):
        @pl.loop(lo, hi)
        def _(i):
            rs = pl.ds(pl.multiple_of(i * RT, RT), RT)
            vh = Vh[rs, :]
            acc = jnp.dot(vh, Tl[...], preferred_element_type=jnp.float32)
            acc += jnp.dot(Vl[rs, :], Th[...], preferred_element_type=jnp.float32)
            acc += jnp.dot(vh, Th[...], preferred_element_type=jnp.float32)
            Pt[u, rs, :] = acc

    def add_at(dst, src, lo, n, off, d0, s0):
        @pl.loop(0, n // 88)
        def _(i):
            rs = pl.ds(pl.multiple_of(lo + i * 88, 8), 88)
            dst[rs, d0:d0 + HB] += src[pl.ds(pl.multiple_of(lo + off + i * 88, 8), 88), s0:s0 + HB]

    def add(dst, srcs, lo, n, d0):
        @pl.loop(0, n // 88)
        def _(i):
            rs = pl.ds(pl.multiple_of(lo + i * 88, 8), 88)
            t = srcs[-1][rs, d0:d0 + HB]
            for s in srcs[:-1]:
                t = t + s[rs, d0:d0 + HB]
            dst[rs, d0:d0 + HB] = t

    def part(k):
        cut = CUT * RT
        return (0, cut) if k == 0 else (cut, rows - cut)

    def half_copy(h, way, i):
        lo, n = CHUNKS[way][i]
        return remote(Pt.at[UNITS.index(("A", h, 0)), pl.ds(lo, n)], RA.at[h * 2 + way, pl.ds(i * RT, n)],
                      hsend.at[h * 2 + way, i], hrecv.at[h * 2 + way, i], r, col_of((1, 3)[way], 0))

    def full_copy(h, way, p, k):
        lo, n = part(k)
        i = h * 2 + way
        return remote(Pt.at[UNITS.index(("M", h, p)), pl.ds(lo, n), pl.ds(way * HB, HB)],
                      RD.at[i, pl.ds(lo, n), pl.ds(p * HB, HB)],
                      xsend.at[i, p * 2 + k], xrecv.at[i, p * 2 + k], r, col_of((1, 3)[way], 0))

    def last_copy(p):
        cs = pl.ds(p * HB, HB)
        return remote(Pt.at[UNITS.index(("D", 1, 0)), :, cs], RY.at[:, cs], lsend.at[p], lrecv.at[p],
                      r, col_of(0, 1))

    def reduce_step(u, k):
        kind, h, p = UNITS[u]
        if kind == "A":
            for i in ((0,), (1,), (2, 3))[k]:
                half_copy(h, 0, i).start()
                half_copy(h, 1, i).start()
        elif kind == "M" and k > 0:
            for way in (0, 1):
                for i in ((0, 1), (2, 3))[k - 1]:
                    if p == 0:
                        half_copy(h, way, i).wait_recv()
                    lo, n = CHUNKS[way][i]
                    add_at(Pt.at[u], RA.at[h * 2 + way], lo, n, i * RT - lo, way * HB, p * HB)
                full_copy(h, way, p, k - 1).start()

    def finish(h, p):
        u = UNITS.index(("D", h, 0))
        for k in (0, 1):
            for way in (0, 1):
                full_copy(h, way, p, k).wait_recv()
        srcs = [RD.at[h * 2], RD.at[h * 2 + 1]]
        if h == 0:
            last_copy(p).wait_recv()
            srcs.append(RY)
        add(out if h == 0 else Pt.at[u], srcs + [Pt.at[u]], 0, rows, p * HB)
        if h == 1:
            last_copy(p).start()

    def unit(u):
        if u > 0:
            E7(u + 1)
            prep(u + 1)
        mm(u, 0, 2)
        reduce_step(u, 0)
        if u == 0:
            mm(u, 2, CUT)
            reduce_step(u, 1)
        if u + 1 < N_UNITS:
            E4(u + 2)
            E5(u + 2)
        if u == 0:
            E2(3)
            E3(3)
            E1(4)
        else:
            mm(u, 2, CUT)
            reduce_step(u, 1)
        mm(u, CUT, n_rt)
        reduce_step(u, 2)
        if u == 5:
            finish(1, 0)
        if u == 6:
            finish(1, 1)
        if u + 1 < N_UNITS:
            E6(u + 2)
        if u + 3 < N_UNITS:
            E2(u + 4)
            E3(u + 4)
        if u + 4 < N_UNITS:
            E1(u + 5)

    a_copy = pltpu.make_async_copy(amp_hbm, amp, asem)
    a_copy.start()
    v_copy(0, 0).start()
    permprep()
    a_copy.wait()
    aprep()
    pl.semaphore_wait(barrier, len(peers))
    send_out(0, 1)
    vprep(0, 3)
    send_out(2, 3, 4)
    T[N_UNITS - 1, slot(z, yl)] = apad[c]
    vprep(3, 4)
    E1(0)
    send_out(5, 6, 7)
    vprep(4, 5)
    E1(1)
    vprep(5, 6)
    E2(0)
    E3(0)
    E2(1)
    E3(1)
    Y0(2)
    vprep(6, 7)
    E5(0)
    E5(1)
    Z0(2)
    E4(0)
    E4(1)
    E6(0)
    E6(1)
    E2(2)
    Y0(3)
    E7(0)
    prep(0)
    E7(1)
    prep(1)
    E3(2)
    Z0(3)
    for u in range(N_UNITS):
        unit(u)
    finish(0, 0)
    for g in range(len(STEPS)):
        if not local(g):
            for i in range(len(a2a_parts(g))):
                a2a(g, i).wait_send()
        for i in (0, 1):
            if i == 0 or g not in NO_Y2:
                ycopy(g, i).wait_send()
            fcopy(g, i).wait_send()
            if g in NO_Y2:
                fcopy(g, i, 1).wait_send()
            for k in (0, 1):
                zcopy(g, i, k).wait_send()
        for i in range(4):
            dcopy(g, i).wait_send()
    for h in (1, 0):
        for way in (0, 1):
            for i in range(4):
                half_copy(h, way, i).wait_send()
                if h == 1 or i < 2:
                    full_copy(h, way, i // 2, i % 2).wait_send()
    last_copy(0).wait_send()
    finish(0, 1)
    last_copy(1).wait_send()
    for way in (0, 1):
        for k in (0, 1):
            full_copy(0, way, 1, k).wait_send()


def per_device(ladder_ints, amplitudes, phase_map):
    rows, depth = ladder_ints.shape
    f32, bf16 = jnp.float32, jnp.bfloat16
    dma = pltpu.SemaphoreType.DMA
    return pl.pallas_call(
        functools.partial(kernel, rows, depth),
        out_shape=pltpu.VMEM((rows, NB), f32),
        in_specs=[pl.BlockSpec(memory_space=pl.ANY), pl.BlockSpec(memory_space=pl.ANY),
                  pl.BlockSpec(memory_space=pltpu.SMEM)],
        out_specs=pl.BlockSpec(memory_space=pltpu.VMEM),
        scratch_shapes=[
            pltpu.VMEM((rows, NB), f32),
            pltpu.VMEM((8, KPAD, NB), f32),
            pltpu.VMEM((256, 256), bf16),
            pltpu.VMEM((N_UNITS, 16, KPAD, NB), f32),
            pltpu.VMEM((rows, KTOT), bf16),
            pltpu.VMEM((rows, KTOT), bf16),
            pltpu.VMEM((KTOT, NB), bf16),
            pltpu.VMEM((KTOT, NB), bf16),
            pltpu.VMEM((N_UNITS, rows, NB), f32),
            pltpu.VMEM((4, rows // 2, NB), f32),
            pltpu.VMEM((4, rows, NB), f32),
            pltpu.VMEM((rows, NB), f32),
            pltpu.VMEM((2, RT, depth), f32),
            dma((9, 2)), dma((9, 2)), dma((9, 2)), dma((9, 2)), dma((9, 4)), dma((9, 4)), dma((9, 4)), dma((9, 4)),
            dma((9, 4)), dma((9, 4)), dma((4, 4)), dma((4, 4)), dma((4, 4)), dma((4, 4)), dma((2,)), dma((2,)),
            dma((2,)), dma,
        ],
        compiler_params=pltpu.CompilerParams(
            collective_id=0, has_side_effects=True, vmem_limit_bytes=65600000),
        name="ladder",
    )(ladder_ints, amplitudes, phase_map)


def solution(mesh):
    in_specs = (P("row", "col"), P("row", "col"), P())
    out_specs = P("row", "col")
    return jax.shard_map(
        per_device, mesh=mesh, in_specs=in_specs, out_specs=out_specs, check_vma=False
    )
```

```python
import functools

import jax
import jax.numpy as jnp
from jax import lax
from jax.experimental import pallas as pl
from jax.experimental.pallas import tpu as pltpu
from jax.sharding import PartitionSpec as P

UNITS = (("A", 1, 0), ("A", 0, 0), ("M", 1, 0), ("M", 1, 1), ("D", 1, 0), ("M", 0, 0), ("M", 0, 1), ("D", 0, 0))
N_UNITS = 8
KPAD = 160
KTOT = 16 * KPAD
NB = 256
HB = NB // 2
RT = 176
CUT = 4
STEPS = ((0, 0, KPAD // 2), (0, KPAD // 2, KPAD // 2)) + tuple((u, 0, KPAD) for u in range(1, N_UNITS))
NO_Y2 = (0, 1, 7, 8)
CHUNKS = (((0, RT), (2 * RT, RT), (4 * RT, RT), (6 * RT, RT // 2)),
          ((RT, RT), (3 * RT, RT), (5 * RT, RT), (6 * RT + RT // 2, RT // 2)))
MESH = pl.DeviceIdType.MESH


def kernel(rows, depth, v_hbm, amp_hbm, phase, out,
           amp, apad, perm, T, Vh, Vl, Th, Tl, Pt, RA, RD, RY, Vs,
           arecv, yrecv, zrecv, frecv, drecv, hrecv, xrecv, lrecv, sent, vsem, asem):
    r = lax.axis_index("row")
    c = lax.axis_index("col")
    x = c // 2
    yh = c % 2
    yl = r // 8
    z = (r // 2) % 4
    core = r % 2
    kb = depth // 16
    n_rt = rows // RT

    def col_of(dx, other):
        return ((x + dx) % 4) * 2 + (yh + other) % 2

    def row_of(other):
        return ((yl + other) % 2) * 8 + z * 2 + core

    row_y = row_of(1)
    zs = (z, (z + 3) % 4, (z + 1) % 4, (z + 2) % 4)
    row_zp = yl * 8 + zs[2] * 2 + core
    row_zm = yl * 8 + zs[1] * 2 + core
    row_z = (row_zp, row_zm)
    row_c = yl * 8 + z * 2 + (core + 1) % 2

    def remote(src, dst, ssem, rsem, row, col):
        return pltpu.make_async_remote_copy(
            src_ref=src, dst_ref=dst, send_sem=ssem, recv_sem=rsem,
            device_id={"row": row, "col": col}, device_id_type=MESH)

    a_copy = pltpu.make_async_copy(amp_hbm, amp, asem)
    a_copy.start()

    barrier = pltpu.get_barrier_semaphore()
    peers = [(row_of(o), col_of(dx, o)) for dx in range(4) for o in (0, 1) if (dx, o) != (0, 0)]
    peers += [(row_y, c), (row_zp, c), (row_zm, c), (row_c, c), (r, col_of(0, 1))]
    for pr, pc in peers:
        pl.semaphore_signal(barrier, inc=1, device_id={"row": pr, "col": pc}, device_id_type=MESH)

    def v_copy(i, slot):
        return pltpu.make_async_copy(v_hbm.at[pl.ds(i * RT, RT), :], Vs.at[slot], vsem.at[slot])

    def own(u):
        return (yl + UNITS[u][1]) % 2

    def slot(zz, ys):
        return core * 8 + zz * 2 + ys

    def piece(g, zz, ys):
        u, lo, n = STEPS[g]
        return T.at[u, slot(zz, ys), pl.ds(lo, n)]

    def a2a_parts(g):
        kind, _, p = UNITS[STEPS[g][0]]
        if kind == "M":
            return ((1, p * HB, HB, 0), (3, p * HB, HB, HB))
        return ((2 if kind == "A" else 0, 0, NB, 0),)

    def a2a(g, i):
        u, lo, n = STEPS[g]
        dx, c0, w, d0 = a2a_parts(g)[i]
        o = UNITS[u][1]
        dcol = col_of(4 - dx, o)
        return remote(apad.at[dcol, pl.ds(lo, n), pl.ds(c0, w)],
                      T.at[u, slot(z, yl), pl.ds(lo, n), pl.ds(d0, w)],
                      sent.at[0], arecv.at[g], row_of(o), dcol)

    def arrival(ref, sem):
        return remote(ref, ref, sent.at[0], sem, r, c)

    def all_sent(ref, k):
        remote(ref, ref, sent.at[k], sent.at[k], r, c).wait_send()

    def send_out(*gs):
        for g in gs:
            for i in range(len(a2a_parts(g))):
                a2a(g, i).start()

    def ycopy(g, i):
        ref = piece(g, zs[3 * i], own(STEPS[g][0]))
        return remote(ref, ref, sent.at[1], yrecv.at[g, i], row_y, c)

    def ycopy_in(g, i):
        ref = piece(g, zs[3 * i], 1 - own(STEPS[g][0]))
        return remote(ref, ref, sent.at[1], yrecv.at[g, i], row_y, c)

    def zcopy(g, way, k):
        ref = piece(g, z, (own(STEPS[g][0]) + k) % 2)
        return remote(ref, ref, sent.at[2], zrecv.at[g, way * 2 + k], row_z[way], c)

    def zcopy_in(g, way, k):
        ref = piece(g, zs[1 + way], (own(STEPS[g][0]) + k) % 2)
        return remote(ref, ref, sent.at[2], zrecv.at[g, way * 2 + k], row_z[way], c)

    def fpart(g, way, zz, k):
        u, lo, n = STEPS[g]
        return T.at[u, slot(zz, (own(u) + k) % 2), pl.ds(lo + way * (n // 2), n // 2)]

    def fcopy(g, way, k=0):
        ref = fpart(g, way, zs[1 + way], k)
        return remote(ref, ref, sent.at[3], frecv.at[g, k], row_z[way], c)

    def fcopy_in(g, k=0):
        return arrival(piece(g, zs[3], (own(STEPS[g][0]) + k) % 2), frecv.at[g, k])

    def dpair(g, i, k):
        u, lo, n = STEPS[g]
        return T.at[u, pl.ds(k * 8 + zs[i] * 2, 2), pl.ds(lo, n)]

    def dcopy(g, i):
        ref = dpair(g, i, core)
        return remote(ref, ref, sent.at[4], drecv.at[g], row_c, c)

    def dcopy_in(g):
        u, lo, n = STEPS[g]
        return arrival(T.at[u, pl.ds((1 - core) * 8, 8), pl.ds(lo, n)], drecv.at[g])

    def local(g):
        return UNITS[STEPS[g][0]][:2] == ("D", 0)

    def Y0(g):
        if not local(g):
            arrival(piece(g, z, own(STEPS[g][0])), arecv.at[g]).wait_recv()
        ycopy(g, 0).start()

    def Z0(g):
        zcopy(g, 0, 0).start()
        zcopy(g, 1, 0).start()

    def E1(g):
        Y0(g)
        Z0(g)

    def E2(g):
        ycopy_in(g, 0).wait_recv()
        zcopy(g, 0, 1).start()
        zcopy(g, 1, 1).start()
        dcopy(g, 0).start()

    def E3(g):
        for way in (0, 1):
            zcopy_in(g, way, 0).wait_recv()
            fcopy(g, way).start()

    def E4(g):
        fcopy_in(g).wait_recv()
        if g not in NO_Y2:
            ycopy(g, 1).start()

    def E5(g):
        for way in (0, 1):
            zcopy_in(g, way, 1).wait_recv()
            if g in NO_Y2:
                fcopy(g, way, 1).start()
            dcopy(g, 1 + way).start()

    def E6(g):
        if g in NO_Y2:
            fcopy_in(g, 1).wait_recv()
        else:
            ycopy_in(g, 1).wait_recv()
        dcopy(g, 3).start()

    def E7(g):
        dcopy_in(g).wait_recv()

    def vprep(lo, hi):
        @pl.loop(lo, hi)
        def _(i):
            s = i % 2

            @pl.when(i + 1 < n_rt)
            def _():
                v_copy(i + 1, (i + 1) % 2).start()

            v_copy(i, s).wait()
            rs = pl.ds(pl.multiple_of(i * RT, RT), RT)
            for j in range(KTOT // 256):
                w = min(256, depth - j * 256)
                v = Vs[s, :, j * 256:j * 256 + w]
                h = v.astype(jnp.bfloat16)
                l = (v - h.astype(jnp.float32)).astype(jnp.bfloat16)
                p = perm[0:w, :]
                Vh[rs, j * 256:(j + 1) * 256] = jnp.dot(h, p, preferred_element_type=jnp.float32).astype(jnp.bfloat16)
                Vl[rs, j * 256:(j + 1) * 256] = jnp.dot(l, p, preferred_element_type=jnp.float32).astype(jnp.bfloat16)

    def aprep():
        for j in range(8):
            apad[j, 0:kb, :] = amp[j * kb:(j + 1) * kb, :]
            apad[j, kb:KPAD, :] = jnp.zeros((KPAD - kb, NB), jnp.float32)

    def permprep():
        lane = lax.broadcasted_iota(jnp.int32, (1, 256), 1)
        want = (lane // 128) * 128 + (lane % 8) * 16
        which = (lane % 128) // 8
        for s in range(16):
            g = (s % 2) * 8 + ((s // 2) % 4) * 2 + s // 8
            want = want + jnp.where(which == s, phase[g], 0)
        rowi = lax.broadcasted_iota(jnp.int32, (256, 256), 0)
        perm[...] = jnp.where(rowi == want, 1.0, 0.0).astype(jnp.bfloat16)

    def prep(g):
        u, first, n = STEPS[g]

        @pl.loop(first // 8, (first + n) // 8)
        def _(k):
            t = T[u, :, pl.ds(pl.multiple_of(k * 8, 8), 8), :].reshape(128, NB)
            h = t.astype(jnp.bfloat16)
            ks = pl.ds(pl.multiple_of(k * 128, 128), 128)
            Th[ks, :] = h
            Tl[ks, :] = (t - h.astype(jnp.float32)).astype(jnp.bfloat16)

    def mm(u, lo, hi):
        @pl.loop(lo, hi)
        def _(i):
            rs = pl.ds(pl.multiple_of(i * RT, RT), RT)
            vh = Vh[rs, :]
            acc = jnp.dot(vh, Tl[...], preferred_element_type=jnp.float32)
            acc += jnp.dot(Vl[rs, :], Th[...], preferred_element_type=jnp.float32)
            acc += jnp.dot(vh, Th[...], preferred_element_type=jnp.float32)
            Pt[u, rs, :] = acc

    def add_at(dst, src, lo, n, off, d0, s0):
        @pl.loop(0, n // 88)
        def _(i):
            rs = pl.ds(pl.multiple_of(lo + i * 88, 8), 88)
            dst[rs, d0:d0 + HB] += src[pl.ds(pl.multiple_of(lo + off + i * 88, 8), 88), s0:s0 + HB]

    def add(dst, srcs, lo, n, d0):
        @pl.loop(0, n // 88)
        def _(i):
            rs = pl.ds(pl.multiple_of(lo + i * 88, 8), 88)
            t = srcs[-1][rs, d0:d0 + HB]
            for s in srcs[:-1]:
                t = t + s[rs, d0:d0 + HB]
            dst[rs, d0:d0 + HB] = t

    def part(k):
        cut = CUT * RT
        return (0, cut) if k == 0 else (cut, rows - cut)

    def half_copy(h, way, i):
        lo, n = CHUNKS[way][i]
        return remote(Pt.at[UNITS.index(("A", h, 0)), pl.ds(lo, n)], RA.at[h * 2 + way, pl.ds(i * RT, n)],
                      sent.at[5], hrecv.at[h * 2 + way, i // 2], r, col_of((1, 3)[way], 0))

    def full_copy(h, way, p, k):
        lo, n = part(k)
        i = h * 2 + way
        return remote(Pt.at[UNITS.index(("M", h, p)), pl.ds(lo, n), pl.ds(way * HB, HB)],
                      RD.at[i, pl.ds(lo, n), pl.ds(p * HB, HB)],
                      sent.at[6], xrecv.at[h, p], r, col_of((1, 3)[way], 0))

    def last_copy(p):
        cs = pl.ds(p * HB, HB)
        return remote(Pt.at[UNITS.index(("D", 1, 0)), :, cs], RY.at[:, cs], sent.at[7], lrecv.at[p],
                      r, col_of(0, 1))

    def reduce_step(u, k):
        kind, h, p = UNITS[u]
        if kind == "A":
            for i in ((0,), (1,), (2, 3))[k]:
                half_copy(h, 0, i).start()
                half_copy(h, 1, i).start()
        elif kind == "M" and k > 0:
            for way in (0, 1):
                if p == 0:
                    rs = ((0, 2 * RT), (2 * RT, RT + RT // 2))[k - 1]
                    arrival(RA.at[h * 2 + way, pl.ds(*rs)], hrecv.at[h * 2 + way, k - 1]).wait_recv()
                for i in ((0, 1), (2, 3))[k - 1]:
                    lo, n = CHUNKS[way][i]
                    add_at(Pt.at[u], RA.at[h * 2 + way], lo, n, i * RT - lo, way * HB, p * HB)
                full_copy(h, way, p, k - 1).start()

    def finish(h, p):
        u = UNITS.index(("D", h, 0))
        arrival(RD.at[pl.ds(h * 2, 2), :, pl.ds(p * HB, HB)], xrecv.at[h, p]).wait_recv()
        srcs = [RD.at[h * 2], RD.at[h * 2 + 1]]
        if h == 0:
            last_copy(p).wait_recv()
            srcs.append(RY)
        add(out if h == 0 else Pt.at[u], srcs + [Pt.at[u]], 0, rows, p * HB)
        if h == 1:
            last_copy(p).start()

    def unit(u):
        if u > 0:
            E7(u + 1)
            prep(u + 1)
        mm(u, 0, 2)
        reduce_step(u, 0)
        if u == 0:
            E3(2)
            Z0(3)
            mm(u, 2, CUT)
            reduce_step(u, 1)
        if u + 1 < N_UNITS:
            E4(u + 2)
            E5(u + 2)
        if u < 2:
            E2(u + 3)
            E3(u + 3)
        if u == 0:
            E1(4)
            E1(5)
        else:
            if u == 1:
                E1(6)
            mm(u, 2, CUT)
            reduce_step(u, 1)
        if u == 6:
            finish(1, 1)
        mm(u, CUT, n_rt)
        reduce_step(u, 2)
        if u == 4:
            finish(1, 0)
        if u + 1 < N_UNITS:
            E6(u + 2)
        if 0 < u < N_UNITS - 3:
            E2(u + 4)
            E3(u + 4)
        if 0 < u < N_UNITS - 5:
            E1(u + 6)

    v_copy(0, 0).start()
    permprep()
    a_copy.wait()
    aprep()
    pl.semaphore_wait(barrier, len(peers))
    send_out(0, 1)
    vprep(0, 3)
    send_out(2, 3, 4)
    T[N_UNITS - 1, slot(z, yl)] = apad[c]
    vprep(3, 4)
    E1(0)
    send_out(5, 6, 7)
    vprep(4, 5)
    E1(1)
    vprep(5, 6)
    E2(0)
    E3(0)
    E2(1)
    E3(1)
    Y0(2)
    vprep(6, 7)
    E5(0)
    E5(1)
    Z0(2)
    E4(0)
    E4(1)
    E6(0)
    E6(1)
    E2(2)
    Y0(3)
    E7(0)
    prep(0)
    E7(1)
    prep(1)
    for u in range(N_UNITS):
        unit(u)
    finish(0, 0)
    all_sent(T.at[0, 0:7], 0)
    all_sent(T.at[0, 0:2 * 8 - len(set(STEPS[g][0] for g in NO_Y2))], 1)
    all_sent(T.at[0:2], 2)
    all_sent(T.at[0, 0:8 + len(set(STEPS[g][0] for g in NO_Y2))], 3)
    all_sent(T.at[0:4], 4)
    all_sent(Pt.at[0:2], 5)
    finish(0, 1)
    all_sent(Pt.at[0:4], 6)
    all_sent(RY, 7)


def per_device(ladder_ints, amplitudes, phase_map):
    rows, depth = ladder_ints.shape
    f32, bf16 = jnp.float32, jnp.bfloat16
    dma = pltpu.SemaphoreType.DMA
    return pl.pallas_call(
        functools.partial(kernel, rows, depth),
        out_shape=pltpu.VMEM((rows, NB), f32),
        in_specs=[pl.BlockSpec(memory_space=pl.ANY), pl.BlockSpec(memory_space=pl.ANY),
                  pl.BlockSpec(memory_space=pltpu.SMEM)],
        out_specs=pl.BlockSpec(memory_space=pltpu.VMEM),
        scratch_shapes=[
            pltpu.VMEM((rows, NB), f32),
            pltpu.VMEM((8, KPAD, NB), f32),
            pltpu.VMEM((256, 256), bf16),
            pltpu.VMEM((N_UNITS, 16, KPAD, NB), f32),
            pltpu.VMEM((rows, KTOT), bf16),
            pltpu.VMEM((rows, KTOT), bf16),
            pltpu.VMEM((KTOT, NB), bf16),
            pltpu.VMEM((KTOT, NB), bf16),
            pltpu.VMEM((N_UNITS, rows, NB), f32),
            pltpu.VMEM((4, rows // 2, NB), f32),
            pltpu.VMEM((4, rows, NB), f32),
            pltpu.VMEM((rows, NB), f32),
            pltpu.VMEM((2, RT, depth), f32),
            dma((9,)), dma((9, 2)), dma((9, 4)), dma((9, 2)), dma((9,)), dma((4, 2)), dma((2, 2)), dma((2,)),
            dma((8,)), dma((2,)), dma,
        ],
        compiler_params=pltpu.CompilerParams(
            collective_id=0, has_side_effects=True, vmem_limit_bytes=65600000),
        name="ladder",
    )(ladder_ints, amplitudes, phase_map)


def solution(mesh):
    in_specs = (P("row", "col"), P("row", "col"), P())
    out_specs = P("row", "col")
    return jax.shard_map(
        per_device, mesh=mesh, in_specs=in_specs, out_specs=out_specs, check_vma=False
    )
```

```python
import functools

import jax
import jax.numpy as jnp
from jax import lax
from jax.experimental import pallas as pl
from jax.experimental.pallas import tpu as pltpu
from jax.sharding import PartitionSpec as P

UNITS = (("A", 1, 0), ("A", 0, 0), ("M", 1, 0), ("M", 1, 1), ("D", 1, 0), ("M", 0, 0), ("M", 0, 1), ("D", 0, 0))
N_UNITS = 8
KPAD = 160
KTOT = 16 * KPAD
NB = 256
HB = NB // 2
RT = 176
CUT = 4
STEPS = ((0, 0, KPAD // 2), (0, KPAD // 2, KPAD // 2)) + tuple((u, 0, KPAD) for u in range(1, N_UNITS))
NO_Y2 = (0, 1, 7, 8)
RH = RT // 2
MESH = pl.DeviceIdType.MESH


def kernel(rows, depth, v_hbm, amp_hbm, phase, out,
           amp, apad, perm, T, Vh, Vl, Th, Tl, Pt, RA, RD, RY, Vs,
           arecv, yrecv, zrecv, frecv, drecv, hrecv, xrecv, lrecv, sent, vsem, asem):
    r = lax.axis_index("row")
    c = lax.axis_index("col")
    x = c // 2
    yh = c % 2
    yl = r // 8
    z = (r // 2) % 4
    core = r % 2
    kb = depth // 16
    n_rt = rows // RT

    def col_of(dx, other):
        return ((x + dx) % 4) * 2 + (yh + other) % 2

    def row_of(other):
        return ((yl + other) % 2) * 8 + z * 2 + core

    row_y = row_of(1)
    zs = (z, (z + 3) % 4, (z + 1) % 4, (z + 2) % 4)
    row_zp = yl * 8 + zs[2] * 2 + core
    row_zm = yl * 8 + zs[1] * 2 + core
    row_z = (row_zp, row_zm)
    row_c = yl * 8 + z * 2 + (core + 1) % 2

    def remote(src, dst, ssem, rsem, row, col):
        return pltpu.make_async_remote_copy(
            src_ref=src, dst_ref=dst, send_sem=ssem, recv_sem=rsem,
            device_id={"row": row, "col": col}, device_id_type=MESH)

    a_copy = pltpu.make_async_copy(amp_hbm, amp, asem)
    a_copy.start()

    barrier = pltpu.get_barrier_semaphore()
    peers = [(row_of(o), col_of(dx, o)) for dx in range(4) for o in (0, 1) if (dx, o) != (0, 0)]
    peers += [(row_y, c), (row_zp, c), (row_zm, c), (row_c, c), (r, col_of(0, 1))]
    for pr, pc in peers:
        pl.semaphore_signal(barrier, inc=1, device_id={"row": pr, "col": pc}, device_id_type=MESH)

    def v_copy(i, slot):
        return pltpu.make_async_copy(v_hbm.at[pl.ds(i * RT, RT), :], Vs.at[slot], vsem.at[slot])

    def own(u):
        return (yl + UNITS[u][1]) % 2

    def slot(zz, ys):
        return core * 8 + zz * 2 + ys

    def piece(g, zz, ys):
        u, lo, n = STEPS[g]
        return T.at[u, slot(zz, ys), pl.ds(lo, n)]

    def a2a_parts(g):
        kind, _, p = UNITS[STEPS[g][0]]
        if kind == "M":
            return ((1, p * HB, HB, 0), (3, p * HB, HB, HB))
        return ((2 if kind == "A" else 0, 0, NB, 0),)

    def a2a(g, i):
        u, lo, n = STEPS[g]
        dx, c0, w, d0 = a2a_parts(g)[i]
        o = UNITS[u][1]
        dcol = col_of(4 - dx, o)
        return remote(apad.at[dcol, pl.ds(lo, n), pl.ds(c0, w)],
                      T.at[u, slot(z, yl), pl.ds(lo, n), pl.ds(d0, w)],
                      sent.at[0], arecv.at[g], row_of(o), dcol)

    def arrival(ref, sem):
        return remote(ref, ref, sent.at[0], sem, r, c)

    def all_sent(ref, k):
        remote(ref, ref, sent.at[k], sent.at[k], r, c).wait_send()

    def send_out(*gs):
        for g in gs:
            for i in range(len(a2a_parts(g))):
                a2a(g, i).start()

    def ycopy(g, i):
        ref = piece(g, zs[3 * i], own(STEPS[g][0]))
        return remote(ref, ref, sent.at[1], yrecv.at[g, i], row_y, c)

    def ycopy_in(g, i):
        ref = piece(g, zs[3 * i], 1 - own(STEPS[g][0]))
        return remote(ref, ref, sent.at[1], yrecv.at[g, i], row_y, c)

    def zcopy(g, way, k):
        ref = piece(g, z, (own(STEPS[g][0]) + k) % 2)
        return remote(ref, ref, sent.at[2], zrecv.at[g, way * 2 + k], row_z[way], c)

    def zcopy_in(g, way, k):
        ref = piece(g, zs[1 + way], (own(STEPS[g][0]) + k) % 2)
        return remote(ref, ref, sent.at[2], zrecv.at[g, way * 2 + k], row_z[way], c)

    def fpart(g, way, zz, k):
        u, lo, n = STEPS[g]
        return T.at[u, slot(zz, (own(u) + k) % 2), pl.ds(lo + way * (n // 2), n // 2)]

    def fcopy(g, way, k=0):
        ref = fpart(g, way, zs[1 + way], k)
        return remote(ref, ref, sent.at[3], frecv.at[g, k], row_z[way], c)

    def fcopy_in(g, k=0):
        return arrival(piece(g, zs[3], (own(STEPS[g][0]) + k) % 2), frecv.at[g, k])

    def dpair(g, i, k):
        u, lo, n = STEPS[g]
        return T.at[u, pl.ds(k * 8 + zs[i] * 2, 2), pl.ds(lo, n)]

    def dcopy(g, i):
        ref = dpair(g, i, core)
        return remote(ref, ref, sent.at[4], drecv.at[g], row_c, c)

    def dcopy_in(g):
        u, lo, n = STEPS[g]
        return arrival(T.at[u, pl.ds((1 - core) * 8, 8), pl.ds(lo, n)], drecv.at[g])

    def local(g):
        return UNITS[STEPS[g][0]][:2] == ("D", 0)

    def Y0(g):
        if not local(g):
            arrival(piece(g, z, own(STEPS[g][0])), arecv.at[g]).wait_recv()
        ycopy(g, 0).start()

    def Z0(g):
        zcopy(g, 0, 0).start()
        zcopy(g, 1, 0).start()

    def E1(g):
        Y0(g)
        Z0(g)

    def E2(g):
        ycopy_in(g, 0).wait_recv()
        zcopy(g, 0, 1).start()
        zcopy(g, 1, 1).start()
        dcopy(g, 0).start()

    def E3(g):
        for way in (0, 1):
            zcopy_in(g, way, 0).wait_recv()
            fcopy(g, way).start()

    def E4(g):
        fcopy_in(g).wait_recv()
        if g not in NO_Y2:
            ycopy(g, 1).start()

    def E5(g):
        for way in (0, 1):
            zcopy_in(g, way, 1).wait_recv()
            if g in NO_Y2:
                fcopy(g, way, 1).start()
            dcopy(g, 1 + way).start()

    def E6(g):
        if g in NO_Y2:
            fcopy_in(g, 1).wait_recv()
        else:
            ycopy_in(g, 1).wait_recv()
        dcopy(g, 3).start()

    def E7(g):
        dcopy_in(g).wait_recv()

    def vprep(lo, hi):
        @pl.loop(lo, hi)
        def _(i):
            s = i % 2

            @pl.when(i + 1 < n_rt)
            def _():
                v_copy(i + 1, (i + 1) % 2).start()

            v_copy(i, s).wait()
            rs = pl.ds(pl.multiple_of(i * RT, RT), RT)
            for j in range(KTOT // 256):
                w = min(256, depth - j * 256)
                v = Vs[s, :, j * 256:j * 256 + w]
                h = v.astype(jnp.bfloat16)
                l = (v - h.astype(jnp.float32)).astype(jnp.bfloat16)
                p = perm[0:w, :]
                Vh[rs, j * 256:(j + 1) * 256] = jnp.dot(h, p, preferred_element_type=jnp.float32).astype(jnp.bfloat16)
                Vl[rs, j * 256:(j + 1) * 256] = jnp.dot(l, p, preferred_element_type=jnp.float32).astype(jnp.bfloat16)

    def aprep():
        for j in range(8):
            apad[j, 0:kb, :] = amp[j * kb:(j + 1) * kb, :]
            apad[j, kb:KPAD, :] = jnp.zeros((KPAD - kb, NB), jnp.float32)

    def permprep():
        lane = lax.broadcasted_iota(jnp.int32, (1, 256), 1)
        want = (lane // 128) * 128 + (lane % 8) * 16
        which = (lane % 128) // 8
        for s in range(16):
            g = (s % 2) * 8 + ((s // 2) % 4) * 2 + s // 8
            want = want + jnp.where(which == s, phase[g], 0)
        rowi = lax.broadcasted_iota(jnp.int32, (256, 256), 0)
        perm[...] = jnp.where(rowi == want, 1.0, 0.0).astype(jnp.bfloat16)

    def prep(g):
        u, first, n = STEPS[g]

        @pl.loop(first // 8, (first + n) // 8)
        def _(k):
            t = T[u, :, pl.ds(pl.multiple_of(k * 8, 8), 8), :].reshape(128, NB)
            h = t.astype(jnp.bfloat16)
            ks = pl.ds(pl.multiple_of(k * 128, 128), 128)
            Th[ks, :] = h
            Tl[ks, :] = (t - h.astype(jnp.float32)).astype(jnp.bfloat16)

    def mm(u, lo, hi):
        @pl.loop(lo, hi)
        def _(i):
            rs = pl.ds(pl.multiple_of(i * RT, RT), RT)
            vh = Vh[rs, :]
            acc = jnp.dot(vh, Tl[...], preferred_element_type=jnp.float32)
            acc += jnp.dot(Vl[rs, :], Th[...], preferred_element_type=jnp.float32)
            acc += jnp.dot(vh, Th[...], preferred_element_type=jnp.float32)
            Pt[u, rs, :] = acc
            if UNITS[u][0] == "A":
                half_copy(UNITS[u][1], 0, i).start()
                half_copy(UNITS[u][1], 1, i).start()

    def add_at(dst, src, lo, n, off, d0, s0):
        @pl.loop(0, n // 88)
        def _(i):
            rs = pl.ds(pl.multiple_of(lo + i * 88, 8), 88)
            dst[rs, d0:d0 + HB] += src[pl.ds(pl.multiple_of(lo + off + i * 88, 8), 88), s0:s0 + HB]

    def add(dst, srcs, lo, n, d0):
        @pl.loop(0, n // 88)
        def _(i):
            rs = pl.ds(pl.multiple_of(lo + i * 88, 8), 88)
            t = srcs[-1][rs, d0:d0 + HB]
            for s in srcs[:-1]:
                t = t + s[rs, d0:d0 + HB]
            dst[rs, d0:d0 + HB] = t

    def part(k):
        cut = CUT * RT
        return (0, cut) if k == 0 else (cut, rows - cut)

    def half_copy(h, way, i):
        return remote(Pt.at[UNITS.index(("A", h, 0)), pl.ds(i * RT + way * RH, RH)],
                      RA.at[h * 2 + way, pl.ds(i * RH, RH)],
                      sent.at[5], hrecv.at[h * 2 + way, i // CUT], r, col_of((1, 3)[way], 0))

    def full_copy(h, way, p, k):
        lo, n = part(k)
        i = h * 2 + way
        return remote(Pt.at[UNITS.index(("M", h, p)), pl.ds(lo, n), pl.ds(way * HB, HB)],
                      RD.at[i, pl.ds(lo, n), pl.ds(p * HB, HB)],
                      sent.at[6], xrecv.at[h, p], r, col_of((1, 3)[way], 0))

    def last_copy(p):
        cs = pl.ds(p * HB, HB)
        return remote(Pt.at[UNITS.index(("D", 1, 0)), :, cs], RY.at[:, cs], sent.at[7], lrecv.at[p],
                      r, col_of(0, 1))

    def reduce_step(u, k):
        kind, h, p = UNITS[u]
        if kind == "M":
            lo, hi = ((0, CUT), (CUT, n_rt))[k]
            for way in (0, 1):
                if p == 0:
                    arrival(RA.at[h * 2 + way, pl.ds(lo * RH, (hi - lo) * RH)], hrecv.at[h * 2 + way, k]).wait_recv()
                for i in range(lo, hi):
                    first = i * RT + way * RH
                    add_at(Pt.at[u], RA.at[h * 2 + way], first, RH, i * RH - first, way * HB, p * HB)
                full_copy(h, way, p, k).start()

    def finish(h, p):
        u = UNITS.index(("D", h, 0))
        arrival(RD.at[pl.ds(h * 2, 2), :, pl.ds(p * HB, HB)], xrecv.at[h, p]).wait_recv()
        srcs = [RD.at[h * 2], RD.at[h * 2 + 1]]
        if h == 0:
            last_copy(p).wait_recv()
            srcs.append(RY)
        add(out if h == 0 else Pt.at[u], srcs + [Pt.at[u]], 0, rows, p * HB)
        if h == 1:
            last_copy(p).start()

    def unit(u):
        if u > 0:
            E7(u + 1)
            prep(u + 1)
        mm(u, 0, 2)
        if u == 0:
            E3(2)
            Z0(3)
            mm(u, 2, CUT)
            E4(2)
            E5(2)
            E2(3)
            mm(u, CUT, n_rt)
            E3(3)
            E1(4)
            E1(5)
            E6(2)
            return
        if u + 1 < N_UNITS:
            E4(u + 2)
            E5(u + 2)
        if u == 1:
            E2(4)
            E3(4)
            E1(6)
        mm(u, 2, CUT)
        reduce_step(u, 0)
        if u == 6:
            finish(1, 1)
        mm(u, CUT, n_rt)
        reduce_step(u, 1)
        if u == 4:
            finish(1, 0)
        if u + 1 < N_UNITS:
            E6(u + 2)
        if u < N_UNITS - 3:
            E2(u + 4)
            E3(u + 4)
        if u < N_UNITS - 6:
            E1(u + 6)

    v_copy(0, 0).start()
    permprep()
    a_copy.wait()
    aprep()
    T[N_UNITS - 1, slot(z, yl)] = apad[c]
    pl.semaphore_wait(barrier, len(peers))
    send_out(0, 1)
    E1(8)
    vprep(0, 3)
    send_out(2, 3, 4)
    vprep(3, 4)
    E1(0)
    send_out(5, 6, 7)
    vprep(4, 5)
    E1(1)
    vprep(5, 6)
    E2(0)
    E3(0)
    E2(1)
    E3(1)
    Y0(2)
    vprep(6, 7)
    E5(0)
    E5(1)
    Z0(2)
    E4(0)
    E4(1)
    E6(0)
    E6(1)
    E2(2)
    Y0(3)
    E7(0)
    prep(0)
    E7(1)
    prep(1)
    for u in range(N_UNITS):
        unit(u)
    finish(0, 0)
    all_sent(T.at[0, 0:7], 0)
    over_z = sum(STEPS[g][2] for g in NO_Y2)
    for rows_sent, k in ((16 * KPAD - over_z, 1), (8 * KPAD + over_z, 3)):
        all_sent(T.at[0, 0:rows_sent // KPAD], k)
        if rows_sent % KPAD:
            all_sent(T.at[0, 0, 0:rows_sent % KPAD], k)
    all_sent(T.at[0:2], 2)
    all_sent(T.at[0:4], 4)
    all_sent(Pt.at[0:2], 5)
    finish(0, 1)
    all_sent(Pt.at[0:4], 6)
    all_sent(RY, 7)


def per_device(ladder_ints, amplitudes, phase_map):
    rows, depth = ladder_ints.shape
    f32, bf16 = jnp.float32, jnp.bfloat16
    dma = pltpu.SemaphoreType.DMA
    return pl.pallas_call(
        functools.partial(kernel, rows, depth),
        out_shape=pltpu.VMEM((rows, NB), f32),
        in_specs=[pl.BlockSpec(memory_space=pl.ANY), pl.BlockSpec(memory_space=pl.ANY),
                  pl.BlockSpec(memory_space=pltpu.SMEM)],
        out_specs=pl.BlockSpec(memory_space=pltpu.VMEM),
        scratch_shapes=[
            pltpu.VMEM((rows, NB), f32),
            pltpu.VMEM((8, KPAD, NB), f32),
            pltpu.VMEM((256, 256), bf16),
            pltpu.VMEM((N_UNITS, 16, KPAD, NB), f32),
            pltpu.VMEM((rows, KTOT), bf16),
            pltpu.VMEM((rows, KTOT), bf16),
            pltpu.VMEM((KTOT, NB), bf16),
            pltpu.VMEM((KTOT, NB), bf16),
            pltpu.VMEM((N_UNITS, rows, NB), f32),
            pltpu.VMEM((4, rows // 2, NB), f32),
            pltpu.VMEM((4, rows, NB), f32),
            pltpu.VMEM((rows, NB), f32),
            pltpu.VMEM((2, RT, depth), f32),
            dma((9,)), dma((9, 2)), dma((9, 4)), dma((9, 2)), dma((9,)), dma((4, 2)), dma((2, 2)), dma((2,)),
            dma((8,)), dma((2,)), dma,
        ],
        compiler_params=pltpu.CompilerParams(
            collective_id=0, has_side_effects=True, vmem_limit_bytes=65600000),
        name="ladder",
    )(ladder_ints, amplitudes, phase_map)


def solution(mesh):
    in_specs = (P("row", "col"), P("row", "col"), P())
    out_specs = P("row", "col")
    return jax.shard_map(
        per_device, mesh=mesh, in_specs=in_specs, out_specs=out_specs, check_vma=False
    )
```

```python
import functools

import jax
import jax.numpy as jnp
from jax import lax
from jax.experimental import pallas as pl
from jax.experimental.pallas import tpu as pltpu
from jax.sharding import PartitionSpec as P

UNITS = (("A", 1, 0), ("A", 0, 0), ("M", 1, 0), ("M", 1, 1), ("D", 1, 0), ("M", 0, 0), ("M", 0, 1), ("D", 0, 0))
N_UNITS = 8
KPAD = 160
KTOT = 16 * KPAD
NB = 256
HB = NB // 2
RT = 176
CUT = 4
STEPS = ((0, 0, KPAD // 2), (0, KPAD // 2, KPAD // 2)) + tuple((u, 0, KPAD) for u in range(1, N_UNITS))
NO_Y2 = (0, 1, 7, 8)
RH = RT // 2
MESH = pl.DeviceIdType.MESH


def kernel(rows, depth, v_hbm, amp_hbm, phase, out,
           amp, apad, perm, T, Vh, Vl, Th, Tl, Pt, RA, RD, RY, Vs,
           arecv, yrecv, zrecv, frecv, drecv, hrecv, xrecv, lrecv, sent, vsem, asem):
    r = lax.axis_index("row")
    c = lax.axis_index("col")
    x = c // 2
    yh = c % 2
    yl = r // 8
    z = (r // 2) % 4
    core = r % 2
    kb = depth // 16
    n_rt = rows // RT

    def col_of(dx, other):
        return ((x + dx) % 4) * 2 + (yh + other) % 2

    def row_of(other):
        return ((yl + other) % 2) * 8 + z * 2 + core

    row_y = row_of(1)
    zs = (z, (z + 3) % 4, (z + 1) % 4, (z + 2) % 4)
    row_zp = yl * 8 + zs[2] * 2 + core
    row_zm = yl * 8 + zs[1] * 2 + core
    row_z = (row_zp, row_zm)
    row_c = yl * 8 + z * 2 + (core + 1) % 2

    def remote(src, dst, ssem, rsem, row, col):
        return pltpu.make_async_remote_copy(
            src_ref=src, dst_ref=dst, send_sem=ssem, recv_sem=rsem,
            device_id={"row": row, "col": col}, device_id_type=MESH)

    a_copy = pltpu.make_async_copy(amp_hbm, amp, asem)
    a_copy.start()

    barrier = pltpu.get_barrier_semaphore()
    peers = [(row_of(o), col_of(dx, o)) for dx in range(4) for o in (0, 1) if (dx, o) != (0, 0)]
    peers += [(row_y, c), (row_zp, c), (row_zm, c), (row_c, c), (r, col_of(0, 1))]
    for pr, pc in peers:
        pl.semaphore_signal(barrier, inc=1, device_id={"row": pr, "col": pc}, device_id_type=MESH)

    def v_copy(i, slot):
        return pltpu.make_async_copy(v_hbm.at[pl.ds(i * RT, RT), :], Vs.at[slot], vsem.at[slot])

    def own(u):
        return (yl + UNITS[u][1]) % 2

    def slot(zz, ys):
        return core * 8 + zz * 2 + ys

    def piece(g, zz, ys):
        u, lo, n = STEPS[g]
        return T.at[u, slot(zz, ys), pl.ds(lo, n)]

    def a2a_parts(g):
        kind, _, p = UNITS[STEPS[g][0]]
        if kind == "M":
            return ((1, p * HB, HB, 0), (3, p * HB, HB, HB))
        return ((2 if kind == "A" else 0, 0, NB, 0),)

    def a2a(g, i):
        u, lo, n = STEPS[g]
        dx, c0, w, d0 = a2a_parts(g)[i]
        o = UNITS[u][1]
        dcol = col_of(4 - dx, o)
        return remote(apad.at[dcol, pl.ds(lo, n), pl.ds(c0, w)],
                      T.at[u, slot(z, yl), pl.ds(lo, n), pl.ds(d0, w)],
                      sent.at[0], arecv.at[g], row_of(o), dcol)

    def arrival(ref, sem):
        return remote(ref, ref, sent.at[0], sem, r, c)

    def all_sent(ref, k):
        remote(ref, ref, sent.at[k], sent.at[k], r, c).wait_send()

    def send_out(*gs):
        for g in gs:
            for i in range(len(a2a_parts(g))):
                a2a(g, i).start()

    def ycopy(g, i):
        ref = piece(g, zs[3 * i], own(STEPS[g][0]))
        return remote(ref, ref, sent.at[1], yrecv.at[g, i], row_y, c)

    def ycopy_in(g, i):
        ref = piece(g, zs[3 * i], 1 - own(STEPS[g][0]))
        return remote(ref, ref, sent.at[1], yrecv.at[g, i], row_y, c)

    def zcopy(g, way, k):
        ref = piece(g, z, (own(STEPS[g][0]) + k) % 2)
        return remote(ref, ref, sent.at[2], zrecv.at[g, way * 2 + k], row_z[way], c)

    def zcopy_in(g, way, k):
        ref = piece(g, zs[1 + way], (own(STEPS[g][0]) + k) % 2)
        return remote(ref, ref, sent.at[2], zrecv.at[g, way * 2 + k], row_z[way], c)

    def fpart(g, way, zz, k):
        u, lo, n = STEPS[g]
        return T.at[u, slot(zz, (own(u) + k) % 2), pl.ds(lo + way * (n // 2), n // 2)]

    def fcopy(g, way, k=0):
        ref = fpart(g, way, zs[1 + way], k)
        return remote(ref, ref, sent.at[3], frecv.at[g, k], row_z[way], c)

    def fcopy_in(g, k=0):
        return arrival(piece(g, zs[3], (own(STEPS[g][0]) + k) % 2), frecv.at[g, k])

    def dpair(g, i, k):
        u, lo, n = STEPS[g]
        return T.at[u, pl.ds(k * 8 + zs[i] * 2, 2), pl.ds(lo, n)]

    def dcopy(g, i):
        ref = dpair(g, i, core)
        return remote(ref, ref, sent.at[4], drecv.at[g], row_c, c)

    def dcopy_in(g):
        u, lo, n = STEPS[g]
        return arrival(T.at[u, pl.ds((1 - core) * 8, 8), pl.ds(lo, n)], drecv.at[g])

    def local(g):
        return UNITS[STEPS[g][0]][:2] == ("D", 0)

    def Y0(g):
        if not local(g):
            arrival(piece(g, z, own(STEPS[g][0])), arecv.at[g]).wait_recv()
        ycopy(g, 0).start()

    def Z0(g):
        zcopy(g, 0, 0).start()
        zcopy(g, 1, 0).start()

    def E1(g):
        Y0(g)
        Z0(g)

    def E2(g):
        ycopy_in(g, 0).wait_recv()
        zcopy(g, 0, 1).start()
        zcopy(g, 1, 1).start()
        dcopy(g, 0).start()

    def E3(g):
        for way in (0, 1):
            zcopy_in(g, way, 0).wait_recv()
            fcopy(g, way).start()

    def E4(g):
        fcopy_in(g).wait_recv()
        if g not in NO_Y2:
            ycopy(g, 1).start()

    def E5(g):
        for way in (0, 1):
            zcopy_in(g, way, 1).wait_recv()
            if g in NO_Y2:
                fcopy(g, way, 1).start()
            dcopy(g, 1 + way).start()

    def E6(g):
        if g in NO_Y2:
            fcopy_in(g, 1).wait_recv()
        else:
            ycopy_in(g, 1).wait_recv()
        dcopy(g, 3).start()

    def E7(g):
        dcopy_in(g).wait_recv()

    def vprep(lo, hi):
        @pl.loop(lo, hi)
        def _(i):
            s = i % 2

            @pl.when(i + 1 < n_rt)
            def _():
                v_copy(i + 1, (i + 1) % 2).start()

            v_copy(i, s).wait()
            rs = pl.ds(pl.multiple_of(i * RT, RT), RT)
            for j in range(KTOT // 256):
                w = min(256, depth - j * 256)
                v = Vs[s, :, j * 256:j * 256 + w]
                h = v.astype(jnp.bfloat16)
                l = (v - h.astype(jnp.float32)).astype(jnp.bfloat16)
                p = perm[0:w, :]
                Vh[rs, j * 256:(j + 1) * 256] = jnp.dot(h, p, preferred_element_type=jnp.float32).astype(jnp.bfloat16)
                Vl[rs, j * 256:(j + 1) * 256] = jnp.dot(l, p, preferred_element_type=jnp.float32).astype(jnp.bfloat16)

    def aprep():
        for j in range(8):
            apad[j, 0:kb, :] = amp[j * kb:(j + 1) * kb, :]
            apad[j, kb:KPAD, :] = jnp.zeros((KPAD - kb, NB), jnp.float32)

    def permprep():
        lane = lax.broadcasted_iota(jnp.int32, (1, 256), 1)
        want = (lane // 128) * 128 + (lane % 8) * 16
        which = (lane % 128) // 8
        for s in range(16):
            g = (s % 2) * 8 + ((s // 2) % 4) * 2 + s // 8
            want = want + jnp.where(which == s, phase[g], 0)
        rowi = lax.broadcasted_iota(jnp.int32, (256, 256), 0)
        perm[...] = jnp.where(rowi == want, 1.0, 0.0).astype(jnp.bfloat16)

    def prep(g):
        u, first, n = STEPS[g]

        @pl.loop(first // 8, (first + n) // 8)
        def _(k):
            t = T[u, :, pl.ds(pl.multiple_of(k * 8, 8), 8), :].reshape(128, NB)
            h = t.astype(jnp.bfloat16)
            ks = pl.ds(pl.multiple_of(k * 128, 128), 128)
            Th[ks, :] = h
            Tl[ks, :] = (t - h.astype(jnp.float32)).astype(jnp.bfloat16)

    def mm(u, lo, hi):
        @pl.loop(lo, hi)
        def _(i):
            rs = pl.ds(pl.multiple_of(i * RT, RT), RT)
            vh = Vh[rs, :]
            acc = jnp.dot(vh, Tl[...], preferred_element_type=jnp.float32)
            acc += jnp.dot(Vl[rs, :], Th[...], preferred_element_type=jnp.float32)
            acc += jnp.dot(vh, Th[...], preferred_element_type=jnp.float32)
            Pt[u, rs, :] = acc
            if UNITS[u][0] == "A":
                half_copy(UNITS[u][1], 0, i).start()
                half_copy(UNITS[u][1], 1, i).start()

    def add_at(dst, src, lo, n, off, d0, s0):
        @pl.loop(0, n // 88)
        def _(i):
            rs = pl.ds(pl.multiple_of(lo + i * 88, 8), 88)
            dst[rs, d0:d0 + HB] += src[pl.ds(pl.multiple_of(lo + off + i * 88, 8), 88), s0:s0 + HB]

    def add(dst, srcs, lo, n, d0):
        @pl.loop(0, n // 88)
        def _(i):
            rs = pl.ds(pl.multiple_of(lo + i * 88, 8), 88)
            t = srcs[-1][rs, d0:d0 + HB]
            for s in srcs[:-1]:
                t = t + s[rs, d0:d0 + HB]
            dst[rs, d0:d0 + HB] = t

    def part(k):
        cut = CUT * RT
        return (0, cut) if k == 0 else (cut, rows - cut)

    def half_copy(h, way, i):
        return remote(Pt.at[UNITS.index(("A", h, 0)), pl.ds(i * RT + way * RH, RH)],
                      RA.at[h * 2 + way, pl.ds(i * RH, RH)],
                      sent.at[5], hrecv.at[h * 2 + way, i // CUT], r, col_of((1, 3)[way], 0))

    def full_copy(h, way, p, k):
        lo, n = part(k)
        i = h * 2 + way
        return remote(Pt.at[UNITS.index(("M", h, p)), pl.ds(lo, n), pl.ds(way * HB, HB)],
                      RD.at[i, pl.ds(lo, n), pl.ds(p * HB, HB)],
                      sent.at[6], xrecv.at[h, p], r, col_of((1, 3)[way], 0))

    def last_copy(p):
        cs = pl.ds(p * HB, HB)
        return remote(Pt.at[UNITS.index(("D", 1, 0)), :, cs], RY.at[:, cs], sent.at[7], lrecv.at[p],
                      r, col_of(0, 1))

    def reduce_step(u, k):
        kind, h, p = UNITS[u]
        if kind == "M":
            lo, hi = ((0, CUT), (CUT, n_rt))[k]
            for way in (0, 1):
                if p == 0:
                    arrival(RA.at[h * 2 + way, pl.ds(lo * RH, (hi - lo) * RH)], hrecv.at[h * 2 + way, k]).wait_recv()
                for i in range(lo, hi):
                    first = i * RT + way * RH
                    add_at(Pt.at[u], RA.at[h * 2 + way], first, RH, i * RH - first, way * HB, p * HB)
                full_copy(h, way, p, k).start()

    def finish(h, p):
        u = UNITS.index(("D", h, 0))
        arrival(RD.at[pl.ds(h * 2, 2), :, pl.ds(p * HB, HB)], xrecv.at[h, p]).wait_recv()
        srcs = [RD.at[h * 2], RD.at[h * 2 + 1]]
        if h == 0:
            last_copy(p).wait_recv()
            srcs.append(RY)
        add(out if h == 0 else Pt.at[u], srcs + [Pt.at[u]], 0, rows, p * HB)
        if h == 1:
            last_copy(p).start()

    def unit(u):
        if u > 0:
            E7(u + 1)
            prep(u + 1)
        mm(u, 0, 2)
        if u == 0:
            E3(2)
            Z0(3)
            mm(u, 2, CUT)
            E4(2)
            E5(2)
            E2(3)
            mm(u, CUT, n_rt)
            E3(3)
            E1(4)
            E1(5)
            E6(2)
            return
        if u + 1 < N_UNITS:
            E4(u + 2)
            E5(u + 2)
        if u == 1:
            E2(4)
            E3(4)
            E1(6)
        mm(u, 2, CUT)
        reduce_step(u, 0)
        if u == 6:
            finish(1, 1)
        mm(u, CUT, n_rt)
        reduce_step(u, 1)
        if u == 4:
            finish(1, 0)
        if u + 1 < N_UNITS:
            E6(u + 2)
        if u < N_UNITS - 3:
            E2(u + 4)
            E3(u + 4)
        if u < N_UNITS - 6:
            E1(u + 6)

    v_copy(0, 0).start()
    permprep()
    a_copy.wait()
    aprep()
    T[N_UNITS - 1, slot(z, yl)] = apad[c]
    pl.semaphore_wait(barrier, len(peers))
    send_out(0, 1)
    E1(8)
    vprep(0, 3)
    send_out(2, 3, 4)
    vprep(3, 4)
    E1(0)
    send_out(5, 6, 7)
    vprep(4, 5)
    E1(1)
    vprep(5, 6)
    E2(0)
    E2(1)
    E3(0)
    E3(1)
    Y0(2)
    vprep(6, 7)
    E5(0)
    E5(1)
    Z0(2)
    E4(0)
    E4(1)
    E6(0)
    E6(1)
    E2(2)
    Y0(3)
    E7(0)
    prep(0)
    E7(1)
    prep(1)
    for u in range(N_UNITS):
        unit(u)
    finish(0, 0)
    all_sent(T.at[0, 0:7], 0)
    over_z = sum(STEPS[g][2] for g in NO_Y2)
    for rows_sent, k in ((16 * KPAD - over_z, 1), (8 * KPAD + over_z, 3)):
        all_sent(T.at[0, 0:rows_sent // KPAD], k)
        if rows_sent % KPAD:
            all_sent(T.at[0, 0, 0:rows_sent % KPAD], k)
    all_sent(T.at[0:2], 2)
    all_sent(T.at[0:4], 4)
    all_sent(Pt.at[0:2], 5)
    finish(0, 1)
    all_sent(Pt.at[0:4], 6)
    all_sent(RY, 7)


def per_device(ladder_ints, amplitudes, phase_map):
    rows, depth = ladder_ints.shape
    f32, bf16 = jnp.float32, jnp.bfloat16
    dma = pltpu.SemaphoreType.DMA
    return pl.pallas_call(
        functools.partial(kernel, rows, depth),
        out_shape=pltpu.VMEM((rows, NB), f32),
        in_specs=[pl.BlockSpec(memory_space=pl.ANY), pl.BlockSpec(memory_space=pl.ANY),
                  pl.BlockSpec(memory_space=pltpu.SMEM)],
        out_specs=pl.BlockSpec(memory_space=pltpu.VMEM),
        scratch_shapes=[
            pltpu.VMEM((rows, NB), f32),
            pltpu.VMEM((8, KPAD, NB), f32),
            pltpu.VMEM((256, 256), bf16),
            pltpu.VMEM((N_UNITS, 16, KPAD, NB), f32),
            pltpu.VMEM((rows, KTOT), bf16),
            pltpu.VMEM((rows, KTOT), bf16),
            pltpu.VMEM((KTOT, NB), bf16),
            pltpu.VMEM((KTOT, NB), bf16),
            pltpu.VMEM((N_UNITS, rows, NB), f32),
            pltpu.VMEM((4, rows // 2, NB), f32),
            pltpu.VMEM((4, rows, NB), f32),
            pltpu.VMEM((rows, NB), f32),
            pltpu.VMEM((2, RT, depth), f32),
            dma((9,)), dma((9, 2)), dma((9, 4)), dma((9, 2)), dma((9,)), dma((4, 2)), dma((2, 2)), dma((2,)),
            dma((8,)), dma((2,)), dma,
        ],
        compiler_params=pltpu.CompilerParams(
            collective_id=0, has_side_effects=True, vmem_limit_bytes=65600000),
        name="ladder",
    )(ladder_ints, amplitudes, phase_map)


def solution(mesh):
    in_specs = (P("row", "col"), P("row", "col"), P())
    out_specs = P("row", "col")
    return jax.shard_map(
        per_device, mesh=mesh, in_specs=in_specs, out_specs=out_specs, check_vma=False
    )
```
